128 devices in a mesh: batch: 1, cols: 16 (over z, y), rows: 8 (over x, core).
Axes of the slice: x: 4, y: 4, z: 4, core: 2. Of those that a mesh axis runs over, the one named last changes fastest.
Arguments:
- frames: bfloat16 [6, 1, 128, 1024, 256], P(None, 'batch', 'rows', 'cols')
- h_init: float32 [1, 128, 1024, 128], P('batch', 'rows', 'cols')
- w_x: bfloat16 [3, 3, 256, 384], replicated
- w_hzr: bfloat16 [3, 3, 128, 256], replicated
- w_hn: bfloat16 [3, 3, 128, 128], replicated
- gate_bias: float32 [384], replicated
Outputs:
- output 1: bfloat16 [6, 1, 128, 1024, 128], P(None, 'batch', 'rows', 'cols')
- output 2: float32 [1, 128, 1024, 128], P('batch', 'rows', 'cols')
All inputs are finite; a program needn't handle non-finite values.
Results may differ from the reference program's by a relative error of at most 0.00239247.
Values are sent between devices in bfloat16 or wider.
A program may use at most 1 GiB of HBM per device.

```python
import jax
import jax.numpy as jnp
from jax import lax

STEPS = 6
BATCH = 1
HEIGHT = 128
WIDTH = 1024
CIN = 256
CH = 128


def setup_inputs(seed: int = 0, part: int = 0) -> dict:
    keys = jax.random.split(jax.random.key(seed), 6)
    key_frames = jax.random.fold_in(keys[0], part)
    key_state = jax.random.fold_in(keys[1], part)
    frames = jax.random.normal(key_frames, (STEPS, BATCH, HEIGHT, WIDTH, CIN), jnp.float32).astype(jnp.bfloat16)
    h_init = 0.8 * jax.random.normal(key_state, (BATCH, HEIGHT, WIDTH, CH), jnp.float32)
    w_x = (jax.random.normal(keys[2], (3, 3, CIN, 3 * CH), jnp.float32) * (9 * CIN) ** -0.5).astype(jnp.bfloat16)
    w_hzr = (jax.random.normal(keys[3], (3, 3, CH, 2 * CH), jnp.float32) * (1.5 * (9 * CH) ** -0.5)).astype(jnp.bfloat16)
    w_hn = (jax.random.normal(keys[4], (3, 3, CH, CH), jnp.float32) * (2.0 * (9 * CH) ** -0.5)).astype(jnp.bfloat16)
    gate_bias = 0.5 * jax.random.normal(keys[5], (3 * CH,), jnp.float32)
    return {'frames': frames, 'h_init': h_init, 'w_x': w_x, 'w_hzr': w_hzr, 'w_hn': w_hn, 'gate_bias': gate_bias}


def conv_same(inputs, weights):
    return lax.conv_general_dilated(inputs.astype(jnp.float32), weights.astype(jnp.float32), (1, 1), 'SAME', dimension_numbers=('NHWC', 'HWIO', 'NHWC'), precision=lax.Precision.HIGHEST)


def reference(frames, h_init, w_x, w_hzr, w_hn, gate_bias):
    def one_step(h_prev, frame_t):
        gate_x = conv_same(frame_t, w_x) + gate_bias
        zr_gates = jax.nn.sigmoid(gate_x[..., :2 * CH] + conv_same(h_prev.astype(jnp.bfloat16), w_hzr))
        update = zr_gates[..., :CH]
        reset_hid = (zr_gates[..., CH:] * h_prev).astype(jnp.bfloat16)
        candidate = jnp.tanh(gate_x[..., 2 * CH:] + conv_same(reset_hid, w_hn))
        h_next = (1.0 - update) * candidate + update * h_prev
        return h_next, h_next.astype(jnp.bfloat16)
    h_last, h_seq = lax.scan(one_step, h_init, frames)
    return h_seq, h_last
```

```python
import functools

import jax
import jax.numpy as jnp
from jax import lax
from jax.experimental import pallas as pl
from jax.experimental.pallas import tpu as pltpu
from jax.sharding import PartitionSpec as P

MESH = pl.DeviceIdType.MESH
F32 = jnp.float32
BF16 = jnp.bfloat16

CH, CIN, SIDE, EDGE, TALL, WIDE = 128, 256, 8, 16, 20, 64
PITCH = 80
BLOCKS = 22
HALF = 11 * PITCH
DIRS = [(dr, dc) for dr in (-1, 0, 1) for dc in (-1, 0, 1) if (dr, dc) != (0, 0)]
EVEN = (PITCH, 736)
ODD = (PITCH, 720)
PAIR = 8 * PITCH + 16
GATE_CHUNK, CAND_CHUNK, ZR_CHUNK, N_CHUNK = 352, 320, 240, 160


def kernel(n_rows, n_cols, steps, refresh, frames, h_init, w_x, w_hzr, w_hn, bias, h_seq, h_last,
           hf, hl, hr, fs, fl, fr, xf, fx, ub, rh, vb, zb, gz, gn, wx, wxn, wh, whn, whr, hs,
           sem_w, sem_f, sem_o, f_send, f_recv, h_send, h_recv):
    row = lax.axis_index('rows')
    col = lax.axis_index('cols')

    def exists(dr, dc):
        conds = []
        if dr:
            conds.append(row + dr >= 0 if dr < 0 else row + dr < n_rows)
        if dc:
            conds.append(col + dc >= 0 if dc < 0 else col + dc < n_cols)
        return conds[0] if len(conds) == 1 else jnp.logical_and(*conds)

    def peer(dr, dc):
        return {'rows': lax.rem(row + dr + n_rows, n_rows), 'cols': lax.rem(col + dc + n_cols, n_cols)}

    def local_copies():
        return [pltpu.make_async_copy(w_x, wx, sem_w.at[0]), pltpu.make_async_copy(w_hzr, wh, sem_w.at[1]),
                pltpu.make_async_copy(w_hn, whr, sem_w.at[2]),
                pltpu.make_async_copy(h_init.at[0], hf.at[0, 3:19, EDGE:PITCH, :], sem_w.at[3])]

    def frame_copy(t):
        return pltpu.make_async_copy(frames.at[t, 0], fs.at[t, 2:18], sem_f.at[t])

    frame_copy(0).start()
    for cp in local_copies():
        cp.start()
    for t in range(1, steps):
        frame_copy(t).start()

    for t in range(steps):
        hf[t, 0, 72:PITCH, :] = jnp.zeros((SIDE, CH), F32)
        hf[t, 1, 0:SIDE, :] = jnp.zeros((SIDE, CH), F32)
        hf[t, 21, SIDE:24, :] = jnp.zeros((EDGE, CH), F32)
    for half in range(2):
        xf[half, 72:88, :] = jnp.zeros((EDGE, CH), F32)
        xf[half, 21 * PITCH + SIDE:21 * PITCH + 24, :] = jnp.zeros((EDGE, CH), F32)

    @pl.when(row == 0)
    def _():
        for t in range(steps):
            hf[t, 1, SIDE:PITCH, :] = jnp.zeros((72, CH), F32)
            hf[t, 2, 0:PITCH, :] = jnp.zeros((PITCH, CH), F32)
            hf[t, 3, 0:SIDE, :] = jnp.zeros((SIDE, CH), F32)
            fs[t, 0:2] = jnp.zeros((2, WIDE, CIN), BF16)
            fl[t, 0:2] = jnp.zeros((2, SIDE, CIN), BF16)
            fr[t, 0:2] = jnp.zeros((2, SIDE, CIN), BF16)
        for s in range(2):
            hl[s, 0:2] = jnp.zeros((2, SIDE, CH), F32)
            hr[s, 0:2] = jnp.zeros((2, SIDE, CH), F32)

    @pl.when(row == n_rows - 1)
    def _():
        for t in range(steps):
            hf[t, 19, SIDE:PITCH, :] = jnp.zeros((72, CH), F32)
            hf[t, TALL, 0:PITCH, :] = jnp.zeros((PITCH, CH), F32)
            hf[t, 21, 0:SIDE, :] = jnp.zeros((SIDE, CH), F32)
            fs[t, 18:TALL] = jnp.zeros((2, WIDE, CIN), BF16)
            fl[t, 18:TALL] = jnp.zeros((2, SIDE, CIN), BF16)
            fr[t, 18:TALL] = jnp.zeros((2, SIDE, CIN), BF16)
        for s in range(2):
            hl[s, 18:TALL] = jnp.zeros((2, SIDE, CH), F32)
            hr[s, 18:TALL] = jnp.zeros((2, SIDE, CH), F32)

    @pl.when(col == 0)
    def _():
        for t in range(steps):
            fl[t] = jnp.zeros((TALL, SIDE, CIN), BF16)
        hl[...] = jnp.zeros((2, TALL, SIDE, CH), F32)

    @pl.when(col == n_cols - 1)
    def _():
        for t in range(steps):
            fr[t] = jnp.zeros((TALL, SIDE, CIN), BF16)
        hr[...] = jnp.zeros((2, TALL, SIDE, CH), F32)

    barrier = pltpu.get_barrier_semaphore()
    count = jnp.int32(0)
    for d in DIRS:
        here = exists(*d)
        count = count + jnp.where(here, 1, 0)

        @pl.when(here)
        def _(d=d):
            pl.semaphore_signal(barrier, inc=1, device_id=peer(*d), device_id_type=MESH)
    pl.semaphore_wait(barrier, count)

    src_y = {-1: slice(0, 2), 0: slice(0, EDGE), 1: slice(14, EDGE)}
    dst_y = {-1: slice(18, TALL), 0: slice(2, 18), 1: slice(0, 2)}

    def frame_xfer(t, i):
        dr, dc = DIRS[i]
        if dc == 0:
            src = frames.at[t, 0, src_y[dr]]
            dst = fs.at[t, dst_y[dr]]
        elif dc == -1:
            src = frames.at[t, 0, src_y[dr], 0:SIDE]
            dst = fr.at[t, dst_y[dr]]
        else:
            src = frames.at[t, 0, src_y[dr], 56:WIDE]
            dst = fl.at[t, dst_y[dr]]
        return pltpu.make_async_remote_copy(src, dst, f_send.at[t, i], f_recv.at[t, i], device_id=peer(dr, dc), device_id_type=MESH)

    def state_xfer(t, i, full, from_arg=False):
        dr, dc = DIRS[i]
        k_src = {-1: slice(3, 5), 0: slice(3, 19), 1: slice(17, 19)}[dr]
        y_src = src_y[dr]
        k_dst = {-1: slice(19, 21), 0: slice(3, 19), 1: slice(1, 3)}[dr]
        if full:
            slot = jnp.where(t == 0, 0, 1)
            if dc == 0:
                xs, dst = slice(EDGE, PITCH), hf.at[t, k_dst, EDGE:PITCH]
            elif dc == -1:
                xs, dst = slice(EDGE, 24), hr.at[slot, dst_y[dr]]
            else:
                xs, dst = slice(72, PITCH), hl.at[slot, dst_y[dr]]
            src = h_init.at[0, y_src, slice(xs.start - EDGE, xs.stop - EDGE)] if from_arg else hf.at[t, k_src, xs]
        else:
            flat = hf.at[t].reshape(BLOCKS * PITCH, CH)
            src = flat.at[pl.ds(PITCH * k_src.start + SIDE, 2 * PITCH)]
            dst = flat.at[pl.ds(PITCH * k_dst.start + SIDE, 2 * PITCH)]
        return pltpu.make_async_remote_copy(src, dst, h_send.at[t, i], h_recv.at[t, i], device_id=peer(dr, dc), device_id_type=MESH)

    def start_frames(t):
        for i, d in enumerate(DIRS):
            @pl.when(exists(*d))
            def _(i=i):
                frame_xfer(t, i).start()

    def wait_frames(t):
        for i, (dr, dc) in enumerate(DIRS):
            @pl.when(exists(dr, dc))
            def _(i=i):
                frame_xfer(t, i).wait_send()

            @pl.when(exists(-dr, -dc))
            def _(i=i):
                frame_xfer(t, i).wait_recv()

    def start_state(t, full, from_arg=False):
        for i, d in enumerate(DIRS):
            if full or d[1] == 0:
                @pl.when(exists(*d))
                def _(i=i):
                    state_xfer(t, i, full, from_arg).start()

    def wait_state(t, full):
        for i, (dr, dc) in enumerate(DIRS):
            if full or dc == 0:
                @pl.when(exists(dr, dc))
                def _(i=i):
                    state_xfer(t, i, full).wait_send()

                @pl.when(exists(-dr, -dc))
                def _(i=i):
                    state_xfer(t, i, full).wait_recv()

    start_frames(0)
    start_state(0, True, True)

    def start_rest(t, carry):
        start_frames(t)
        return carry

    lax.fori_loop(1, steps, start_rest, 0)

    for cp in local_copies():
        cp.wait()
    for c in range(3):
        for a in range(4):
            i = a * 3 + c
            wxn[i * CIN:(i + 1) * CIN, 0:CH] = wx[a * 3 + c, :, CIN:384] if a < 3 else jnp.zeros((CIN, CH), BF16)
            wxn[i * CIN:(i + 1) * CIN, CH:CIN] = wx[(a - 1) * 3 + c, :, CIN:384] if a > 0 else jnp.zeros((CIN, CH), BF16)
            whn[i * CH:(i + 1) * CH, 0:CH] = whr[a * 3 + c] if a < 3 else jnp.zeros((CH, CH), BF16)
            whn[i * CH:(i + 1) * CH, CH:CIN] = whr[(a - 1) * 3 + c] if a > 0 else jnp.zeros((CH, CH), BF16)

    tap_blocks = {0: [(1, -PITCH), (0, 0), (1, 0)], 1: [(0, 0), (1, 0), (0, PITCH)]}
    pair_blocks = [(0, PITCH), (1, PITCH), (0, 2 * PITCH), (1, 2 * PITCH)]

    def patches(ref, blocks, lo, size):
        return jnp.concatenate([ref[c, par, lo + off:lo + off + size, :] for par, off in blocks for c in range(3)], axis=1)

    def chunks(lo, size, step):
        n = size // step
        return [(lo + i * step, step if i < n - 1 else size - i * step) for i in range(n)]

    def paired(step):
        both = zip(chunks(*EVEN, step), chunks(*ODD, step))
        return [(par,) + c for pair in both for par, c in enumerate(pair)]

    def gate_conv(t):
        for k in range(1, 21):
            for half in range(2):
                lanes = slice(half * CH, half * CH + CH)
                xf[half, PITCH * k + EDGE:PITCH * k + PITCH, :] = fs[t, k - 1, :, lanes].astype(F32)
                xf[half, PITCH * k + SIDE:PITCH * k + EDGE, :] = fl[t, k - 1, :, lanes].astype(F32)
                xf[half, PITCH * k + PITCH:PITCH * k + 88, :] = fr[t, k - 1, :, lanes].astype(F32)
        for k in range(1, 22):
            width = PITCH if k < 21 else EDGE
            for half in range(2):
                for c in range(3):
                    fx[c, k % 2, (k // 2) * PITCH:(k // 2) * PITCH + width, half * CH:half * CH + CH] = (
                        xf[half, PITCH * k - 1 + c:PITCH * k - 1 + c + width, :].astype(BF16))
        bias_zr = bias[0:CIN][None, :]
        wzr = wx[:, :, 0:CIN].reshape(9 * CIN, CIN)
        for par, lo, size in paired(GATE_CHUNK):
                gz[par, lo:lo + size, :] = jnp.dot(patches(fx, tap_blocks[par], lo, size), wzr, preferred_element_type=F32) + bias_zr
        bias_n = jnp.concatenate([bias[CIN:384], bias[CIN:384]])[None, :]
        for lo, size in chunks(0, PAIR, CAND_CHUNK):
            gn[lo:lo + size, :] = jnp.dot(patches(fx, pair_blocks, lo, size), wxn[...], preferred_element_type=F32) + bias_n

    left_edge = col == 0
    right_edge = col == n_cols - 1

    def step(t, carry):
        frame_copy(t).wait()
        wait_frames(t)
        gate_conv(t)
        is_full = jnp.logical_or(t == 0, t == refresh)

        @pl.when(is_full)
        def _():
            wait_state(t, True)
            slot = jnp.where(t == 0, 0, 1)
            for y in range(TALL):
                hf[t, y + 1, SIDE:EDGE, :] = hl[slot, y]
                hf[t, y + 2, 0:SIDE, :] = hr[slot, y]

        @pl.when(jnp.logical_not(is_full))
        def _():
            wait_state(t, False)

        h_flat = hf.at[t].reshape(BLOCKS * PITCH, CH)
        for k in range(1, 22):
            width = PITCH if k < 21 else EDGE
            for c in range(3):
                ub[c, k % 2, (k // 2) * PITCH:(k // 2) * PITCH + width, :] = h_flat[PITCH * k - 1 + c:PITCH * k - 1 + c + width, :].astype(BF16)

        whzr = wh[...].reshape(9 * CH, CIN)
        for par, lo, size in paired(ZR_CHUNK):
                pre = jnp.dot(patches(ub, tap_blocks[par], lo, size), whzr, preferred_element_type=F32) + gz[par, lo:lo + size, :]
                gate = 0.5 * jnp.tanh(0.5 * pre) + 0.5
                zb[par, lo:lo + size, :] = gate[:, 0:CH]
                for s in range(0, size, PITCH):
                    k = 2 * ((lo + s) // PITCH) + par
                    width = min(PITCH, size - s)
                    rh[PITCH * k:PITCH * k + width, :] = gate[s:s + width, CH:CIN] * h_flat[PITCH * k:PITCH * k + width, :]
        for k in range(2, 21):
            width = PITCH if k < TALL else EDGE
            for c in range(3):
                vb[c, k % 2, (k // 2) * PITCH:(k // 2) * PITCH + width, :] = rh[PITCH * k - 1 + c:PITCH * k - 1 + c + width, :].astype(BF16)

        last = t == steps - 1
        next_full = t + 1 == refresh
        keep_border = jnp.logical_not(jnp.logical_or(last, next_full))
        for lo, size in chunks(0, PAIR, N_CHUNK):
            cand = jnp.tanh(jnp.dot(patches(vb, pair_blocks, lo, size), whn[...], preferred_element_type=F32) + gn[lo:lo + size, :])
            for s in range(0, size, PITCH):
                yy = (lo + s) // PITCH
                width = min(PITCH, size - s)
                for odd in range(2):
                    k = 2 * yy + 3 + odd
                    if width < PITCH and odd:
                        continue
                    z_lo = (k // 2) * PITCH
                    z = zb[k % 2, z_lo:z_lo + width, :]
                    h_new = (1.0 - z) * cand[s:s + width, odd * CH:odd * CH + CH] + z * h_flat[PITCH * k:PITCH * k + width, :]
                    if width == PITCH:
                        main = h_new[EDGE:PITCH]
                        hs[t, k - 3] = main.astype(BF16)
                        hf[t + 1, k, EDGE:PITCH, :] = main
                        hf[t + 1, k, SIDE:EDGE, :] = jnp.where(left_edge, 0.0, h_new[SIDE:EDGE])
                    if k > 3:
                        hf[t + 1, k, 0:SIDE, :] = jnp.where(right_edge, 0.0, h_new[0:SIDE])

        @pl.when(next_full)
        def _():
            start_state(t + 1, True)

        @pl.when(keep_border)
        def _():
            start_state(t + 1, False)

        pltpu.make_async_copy(hs.at[t], h_seq.at[t, 0], sem_o.at[t]).start()
        return carry

    for par, lo in ((1, 10 * PITCH), (0, 10 * PITCH)):
        for c in range(3):
            vb[c, par, lo:lo + EDGE, :] = jnp.zeros((EDGE, CH), BF16)
    rh[2 * PITCH - SIDE:2 * PITCH, :] = jnp.zeros((SIDE, CH), F32)
    rh[TALL * PITCH + EDGE:TALL * PITCH + 24, :] = jnp.zeros((SIDE, CH), F32)
    lax.fori_loop(0, steps, step, 0)
    last_copy = pltpu.make_async_copy(hf.at[steps, 3:19, EDGE:PITCH, :], h_last.at[0], sem_w.at[0])
    last_copy.start()
    for t in range(steps):
        pltpu.make_async_copy(hs.at[t], h_seq.at[t, 0], sem_o.at[t]).wait()
    last_copy.wait()


def solution(mesh):
    n_rows = mesh.shape['rows']
    n_cols = mesh.shape['cols']
    frame_spec = P(None, 'batch', 'rows', 'cols', None)
    state_spec = P('batch', 'rows', 'cols', None)

    def local_fn(frames, h_init, w_x, w_hzr, w_hn, gate_bias):
        steps = frames.shape[0]
        any_spec = pl.BlockSpec(memory_space=pl.ANY)
        vmem = pltpu.VMEM
        dma = pltpu.SemaphoreType.DMA
        return pl.pallas_call(
            functools.partial(kernel, n_rows, n_cols, steps, 3),
            out_shape=(jax.ShapeDtypeStruct((steps, 1, EDGE, WIDE, CH), BF16), jax.ShapeDtypeStruct((1, EDGE, WIDE, CH), F32)),
            in_specs=[any_spec] * 5 + [pl.BlockSpec(memory_space=pltpu.VMEM)],
            out_specs=(any_spec, any_spec),
            scratch_shapes=[
                vmem((steps + 1, BLOCKS, PITCH, CH), F32),
                vmem((2, TALL, SIDE, CH), F32),
                vmem((2, TALL, SIDE, CH), F32),
                vmem((steps, TALL, WIDE, CIN), BF16),
                vmem((steps, TALL, SIDE, CIN), BF16),
                vmem((steps, TALL, SIDE, CIN), BF16),
                vmem((2, BLOCKS * PITCH, CH), F32),
                vmem((3, 2, HALF, CIN), BF16),
                vmem((3, 2, HALF, CH), BF16),
                vmem((BLOCKS * PITCH, CH), F32),
                vmem((3, 2, HALF, CH), BF16),
                vmem((2, HALF, CH), F32),
                vmem((2, HALF, CIN), F32),
                vmem((PAIR, CIN), F32),
                vmem((9, CIN, 384), BF16),
                vmem((12 * CIN, CIN), BF16),
                vmem((9, CH, CIN), BF16),
                vmem((12 * CH, CIN), BF16),
                vmem((9, CH, CH), BF16),
                vmem((steps, EDGE, WIDE, CH), BF16),
                dma((4,)), dma((steps,)), dma((steps,)),
                dma((steps, SIDE)), dma((steps, SIDE)), dma((steps, SIDE)), dma((steps, SIDE)),
            ],
            compiler_params=pltpu.CompilerParams(collective_id=0, has_side_effects=True, vmem_limit_bytes=60 * 1024 * 1024),
        )(frames, h_init, w_x.reshape(9, CIN, 384), w_hzr.reshape(9, CH, CIN), w_hn.reshape(9, CH, CH), gate_bias)

    return jax.shard_map(local_fn, mesh=mesh, in_specs=(frame_spec, state_spec, P(), P(), P(), P()), out_specs=(frame_spec, state_spec), check_vma=False)
```

```python
import functools

import jax
import jax.numpy as jnp
from jax import lax
from jax.experimental import pallas as pl
from jax.experimental.pallas import tpu as pltpu
from jax.sharding import PartitionSpec as P

MESH = pl.DeviceIdType.MESH
F32 = jnp.float32
BF16 = jnp.bfloat16

CH, CIN, SIDE, EDGE, TALL, WIDE = 128, 256, 8, 16, 20, 64
PITCH = 80
BLOCKS = 22
HALF = 11 * PITCH
DIRS = [(dr, dc) for dr in (-1, 0, 1) for dc in (-1, 0, 1) if (dr, dc) != (0, 0)]
EVEN = (PITCH, 736)
ODD = (PITCH, 720)
PAIR = 8 * PITCH + 16
GATE_CHUNK, CAND_CHUNK, ZR_CHUNK, N_CHUNK = 352, 320, 240, 160


def kernel(n_rows, n_cols, steps, refresh, frames, h_init, w_x, w_hzr, w_hn, bias, h_seq, h_last,
           hf, hl, hr, fs, fl, fr, xf, fx, ub, rh, vb, zb, gz, gn, wx, wxn, wh, whn, whr,
           sem_w, sem_f, f_send, f_recv, h_send, h_recv):
    row = lax.axis_index('rows')
    col = lax.axis_index('cols')

    def exists(dr, dc):
        conds = []
        if dr:
            conds.append(row + dr >= 0 if dr < 0 else row + dr < n_rows)
        if dc:
            conds.append(col + dc >= 0 if dc < 0 else col + dc < n_cols)
        return conds[0] if len(conds) == 1 else jnp.logical_and(*conds)

    def peer(dr, dc):
        return {'rows': lax.rem(row + dr + n_rows, n_rows), 'cols': lax.rem(col + dc + n_cols, n_cols)}

    def local_copies():
        return [pltpu.make_async_copy(w_x, wx, sem_w.at[0]), pltpu.make_async_copy(w_hzr, wh, sem_w.at[1]),
                pltpu.make_async_copy(w_hn, whr, sem_w.at[2]),
                pltpu.make_async_copy(h_init.at[0], hf.at[0, 3:19, EDGE:PITCH, :], sem_w.at[3])]

    def frame_copy(t):
        return pltpu.make_async_copy(frames.at[t, 0], fs.at[t, 2:18], sem_f.at[t])

    frame_copy(0).start()
    for cp in local_copies():
        cp.start()
    for t in range(1, steps):
        frame_copy(t).start()

    for t in range(steps):
        hf[t, 0, 72:PITCH, :] = jnp.zeros((SIDE, CH), F32)
        hf[t, 1, 0:SIDE, :] = jnp.zeros((SIDE, CH), F32)
        hf[t, 21, SIDE:24, :] = jnp.zeros((EDGE, CH), F32)
    for half in range(2):
        xf[half, 72:88, :] = jnp.zeros((EDGE, CH), F32)
        xf[half, 21 * PITCH + SIDE:21 * PITCH + 24, :] = jnp.zeros((EDGE, CH), F32)

    @pl.when(row == 0)
    def _():
        for t in range(steps):
            hf[t, 1, SIDE:PITCH, :] = jnp.zeros((72, CH), F32)
            hf[t, 2, 0:PITCH, :] = jnp.zeros((PITCH, CH), F32)
            hf[t, 3, 0:SIDE, :] = jnp.zeros((SIDE, CH), F32)
            fs[t, 0:2] = jnp.zeros((2, WIDE, CIN), BF16)
            fl[t, 0:2] = jnp.zeros((2, SIDE, CIN), BF16)
            fr[t, 0:2] = jnp.zeros((2, SIDE, CIN), BF16)
        for s in range(2):
            hl[s, 0:2] = jnp.zeros((2, SIDE, CH), F32)
            hr[s, 0:2] = jnp.zeros((2, SIDE, CH), F32)

    @pl.when(row == n_rows - 1)
    def _():
        for t in range(steps):
            hf[t, 19, SIDE:PITCH, :] = jnp.zeros((72, CH), F32)
            hf[t, TALL, 0:PITCH, :] = jnp.zeros((PITCH, CH), F32)
            hf[t, 21, 0:SIDE, :] = jnp.zeros((SIDE, CH), F32)
            fs[t, 18:TALL] = jnp.zeros((2, WIDE, CIN), BF16)
            fl[t, 18:TALL] = jnp.zeros((2, SIDE, CIN), BF16)
            fr[t, 18:TALL] = jnp.zeros((2, SIDE, CIN), BF16)
        for s in range(2):
            hl[s, 18:TALL] = jnp.zeros((2, SIDE, CH), F32)
            hr[s, 18:TALL] = jnp.zeros((2, SIDE, CH), F32)

    @pl.when(col == 0)
    def _():
        for t in range(steps):
            fl[t] = jnp.zeros((TALL, SIDE, CIN), BF16)
        hl[...] = jnp.zeros((2, TALL, SIDE, CH), F32)

    @pl.when(col == n_cols - 1)
    def _():
        for t in range(steps):
            fr[t] = jnp.zeros((TALL, SIDE, CIN), BF16)
        hr[...] = jnp.zeros((2, TALL, SIDE, CH), F32)

    barrier = pltpu.get_barrier_semaphore()
    count = jnp.int32(0)
    for d in DIRS:
        here = exists(*d)
        count = count + jnp.where(here, 1, 0)

        @pl.when(here)
        def _(d=d):
            pl.semaphore_signal(barrier, inc=1, device_id=peer(*d), device_id_type=MESH)
    pl.semaphore_wait(barrier, count)

    src_y = {-1: slice(0, 2), 0: slice(0, EDGE), 1: slice(14, EDGE)}
    dst_y = {-1: slice(18, TALL), 0: slice(2, 18), 1: slice(0, 2)}

    def frame_xfer(t, i):
        dr, dc = DIRS[i]
        if dc == 0:
            src = frames.at[t, 0, src_y[dr]]
            dst = fs.at[t, dst_y[dr]]
        elif dc == -1:
            src = frames.at[t, 0, src_y[dr], 0:SIDE]
            dst = fr.at[t, dst_y[dr]]
        else:
            src = frames.at[t, 0, src_y[dr], 56:WIDE]
            dst = fl.at[t, dst_y[dr]]
        return pltpu.make_async_remote_copy(src, dst, f_send.at[t, i], f_recv.at[t, i], device_id=peer(dr, dc), device_id_type=MESH)

    def state_xfer(t, i, full, from_arg=False):
        dr, dc = DIRS[i]
        k_src = {-1: slice(3, 5), 0: slice(3, 19), 1: slice(17, 19)}[dr]
        y_src = src_y[dr]
        k_dst = {-1: slice(19, 21), 0: slice(3, 19), 1: slice(1, 3)}[dr]
        if full:
            slot = jnp.where(t == 0, 0, 1)
            if dc == 0:
                xs, dst = slice(EDGE, PITCH), hf.at[t, k_dst, EDGE:PITCH]
            elif dc == -1:
                xs, dst = slice(EDGE, 24), hr.at[slot, dst_y[dr]]
            else:
                xs, dst = slice(72, PITCH), hl.at[slot, dst_y[dr]]
            src = h_init.at[0, y_src, slice(xs.start - EDGE, xs.stop - EDGE)] if from_arg else hf.at[t, k_src, xs]
        else:
            flat = hf.at[t].reshape(BLOCKS * PITCH, CH)
            src = flat.at[pl.ds(PITCH * k_src.start + SIDE, 2 * PITCH)]
            dst = flat.at[pl.ds(PITCH * k_dst.start + SIDE, 2 * PITCH)]
        return pltpu.make_async_remote_copy(src, dst, h_send.at[t, i], h_recv.at[t, i], device_id=peer(dr, dc), device_id_type=MESH)

    def start_frames(t):
        for i, d in enumerate(DIRS):
            @pl.when(exists(*d))
            def _(i=i):
                frame_xfer(t, i).start()

    def wait_frames(t):
        for i, (dr, dc) in enumerate(DIRS):
            @pl.when(exists(dr, dc))
            def _(i=i):
                frame_xfer(t, i).wait_send()

            @pl.when(exists(-dr, -dc))
            def _(i=i):
                frame_xfer(t, i).wait_recv()

    def start_state(t, full, from_arg=False):
        for i, d in enumerate(DIRS):
            if full or d[1] == 0:
                @pl.when(exists(*d))
                def _(i=i):
                    state_xfer(t, i, full, from_arg).start()

    def wait_state(t, full):
        for i, (dr, dc) in enumerate(DIRS):
            if full or dc == 0:
                @pl.when(exists(dr, dc))
                def _(i=i):
                    state_xfer(t, i, full).wait_send()

                @pl.when(exists(-dr, -dc))
                def _(i=i):
                    state_xfer(t, i, full).wait_recv()

    start_frames(0)
    start_state(0, True, True)

    def start_rest(t, carry):
        start_frames(t)
        return carry

    lax.fori_loop(1, steps, start_rest, 0)

    for cp in local_copies():
        cp.wait()
    for c in range(3):
        for a in range(4):
            i = a * 3 + c
            wxn[i * CIN:(i + 1) * CIN, 0:CH] = wx[a * 3 + c, :, CIN:384] if a < 3 else jnp.zeros((CIN, CH), BF16)
            wxn[i * CIN:(i + 1) * CIN, CH:CIN] = wx[(a - 1) * 3 + c, :, CIN:384] if a > 0 else jnp.zeros((CIN, CH), BF16)
            whn[i * CH:(i + 1) * CH, 0:CH] = whr[a * 3 + c] if a < 3 else jnp.zeros((CH, CH), BF16)
            whn[i * CH:(i + 1) * CH, CH:CIN] = whr[(a - 1) * 3 + c] if a > 0 else jnp.zeros((CH, CH), BF16)

    tap_blocks = {0: [(1, -PITCH), (0, 0), (1, 0)], 1: [(0, 0), (1, 0), (0, PITCH)]}
    pair_blocks = [(0, PITCH), (1, PITCH), (0, 2 * PITCH), (1, 2 * PITCH)]

    def patches(ref, blocks, lo, size):
        return jnp.concatenate([ref[c, par, lo + off:lo + off + size, :] for par, off in blocks for c in range(3)], axis=1)

    def chunks(lo, size, step):
        n = size // step
        return [(lo + i * step, step if i < n - 1 else size - i * step) for i in range(n)]

    def paired(step):
        both = zip(chunks(*EVEN, step), chunks(*ODD, step))
        return [(par,) + c for pair in both for par, c in enumerate(pair)]

    def gate_conv(t):
        for k in range(1, 21):
            for half in range(2):
                lanes = slice(half * CH, half * CH + CH)
                xf[half, PITCH * k + EDGE:PITCH * k + PITCH, :] = fs[t, k - 1, :, lanes].astype(F32)
                xf[half, PITCH * k + SIDE:PITCH * k + EDGE, :] = fl[t, k - 1, :, lanes].astype(F32)
                xf[half, PITCH * k + PITCH:PITCH * k + 88, :] = fr[t, k - 1, :, lanes].astype(F32)
        for k in range(1, 22):
            width = PITCH if k < 21 else EDGE
            for half in range(2):
                for c in range(3):
                    fx[c, k % 2, (k // 2) * PITCH:(k // 2) * PITCH + width, half * CH:half * CH + CH] = (
                        xf[half, PITCH * k - 1 + c:PITCH * k - 1 + c + width, :].astype(BF16))
        bias_zr = bias[0:CIN][None, :]
        wzr = wx[:, :, 0:CIN].reshape(9 * CIN, CIN)
        for par, lo, size in paired(GATE_CHUNK):
                gz[par, lo:lo + size, :] = jnp.dot(patches(fx, tap_blocks[par], lo, size), wzr, preferred_element_type=F32) + bias_zr
        bias_n = jnp.concatenate([bias[CIN:384], bias[CIN:384]])[None, :]
        for lo, size in chunks(0, PAIR, CAND_CHUNK):
            gn[lo:lo + size, :] = jnp.dot(patches(fx, pair_blocks, lo, size), wxn[...], preferred_element_type=F32) + bias_n

    left_edge = col == 0
    right_edge = col == n_cols - 1

    def step(t, carry):
        frame_copy(t).wait()
        wait_frames(t)
        gate_conv(t)
        is_full = jnp.logical_or(t == 0, t == refresh)

        @pl.when(is_full)
        def _():
            wait_state(t, True)
            slot = jnp.where(t == 0, 0, 1)
            for y in range(TALL):
                hf[t, y + 1, SIDE:EDGE, :] = hl[slot, y]
                hf[t, y + 2, 0:SIDE, :] = hr[slot, y]

        @pl.when(jnp.logical_not(is_full))
        def _():
            wait_state(t, False)

        h_flat = hf.at[t].reshape(BLOCKS * PITCH, CH)
        for k in range(1, 22):
            width = PITCH if k < 21 else EDGE
            for c in range(3):
                ub[c, k % 2, (k // 2) * PITCH:(k // 2) * PITCH + width, :] = h_flat[PITCH * k - 1 + c:PITCH * k - 1 + c + width, :].astype(BF16)

        whzr = wh[...].reshape(9 * CH, CIN)
        for par, lo, size in paired(ZR_CHUNK):
                pre = jnp.dot(patches(ub, tap_blocks[par], lo, size), whzr, preferred_element_type=F32) + gz[par, lo:lo + size, :]
                gate = 0.5 * jnp.tanh(0.5 * pre) + 0.5
                zb[par, lo:lo + size, :] = gate[:, 0:CH]
                for s in range(0, size, PITCH):
                    k = 2 * ((lo + s) // PITCH) + par
                    width = min(PITCH, size - s)
                    rh[PITCH * k:PITCH * k + width, :] = gate[s:s + width, CH:CIN] * h_flat[PITCH * k:PITCH * k + width, :]
        for k in range(2, 21):
            width = PITCH if k < TALL else EDGE
            for c in range(3):
                vb[c, k % 2, (k // 2) * PITCH:(k // 2) * PITCH + width, :] = rh[PITCH * k - 1 + c:PITCH * k - 1 + c + width, :].astype(BF16)

        last = t == steps - 1
        next_full = t + 1 == refresh
        keep_border = jnp.logical_not(jnp.logical_or(last, next_full))
        for lo, size in chunks(0, PAIR, N_CHUNK):
            cand = jnp.tanh(jnp.dot(patches(vb, pair_blocks, lo, size), whn[...], preferred_element_type=F32) + gn[lo:lo + size, :])
            for s in range(0, size, PITCH):
                yy = (lo + s) // PITCH
                width = min(PITCH, size - s)
                for odd in range(2):
                    k = 2 * yy + 3 + odd
                    if width < PITCH and odd:
                        continue
                    z_lo = (k // 2) * PITCH
                    z = zb[k % 2, z_lo:z_lo + width, :]
                    h_new = (1.0 - z) * cand[s:s + width, odd * CH:odd * CH + CH] + z * h_flat[PITCH * k:PITCH * k + width, :]
                    if width == PITCH:
                        main = h_new[EDGE:PITCH]
                        h_seq[t, 0, k - 3] = main.astype(BF16)
                        h_last[0, k - 3] = main
                        hf[t + 1, k, EDGE:PITCH, :] = main
                        hf[t + 1, k, SIDE:EDGE, :] = jnp.where(left_edge, 0.0, h_new[SIDE:EDGE])
                    if k > 3:
                        hf[t + 1, k, 0:SIDE, :] = jnp.where(right_edge, 0.0, h_new[0:SIDE])

        @pl.when(next_full)
        def _():
            start_state(t + 1, True)

        @pl.when(keep_border)
        def _():
            start_state(t + 1, False)

        return carry

    for par, lo in ((1, 10 * PITCH), (0, 10 * PITCH)):
        for c in range(3):
            vb[c, par, lo:lo + EDGE, :] = jnp.zeros((EDGE, CH), BF16)
    rh[2 * PITCH - SIDE:2 * PITCH, :] = jnp.zeros((SIDE, CH), F32)
    rh[TALL * PITCH + EDGE:TALL * PITCH + 24, :] = jnp.zeros((SIDE, CH), F32)
    lax.fori_loop(0, steps, step, 0)


def solution(mesh):
    n_rows = mesh.shape['rows']
    n_cols = mesh.shape['cols']
    frame_spec = P(None, 'batch', 'rows', 'cols', None)
    state_spec = P('batch', 'rows', 'cols', None)

    def local_fn(frames, h_init, w_x, w_hzr, w_hn, gate_bias):
        steps = frames.shape[0]
        any_spec = pl.BlockSpec(memory_space=pl.ANY)
        vmem = pltpu.VMEM
        dma = pltpu.SemaphoreType.DMA
        return pl.pallas_call(
            functools.partial(kernel, n_rows, n_cols, steps, 3),
            out_shape=(vmem((steps, 1, EDGE, WIDE, CH), BF16), vmem((1, EDGE, WIDE, CH), F32)),
            in_specs=[any_spec] * 5 + [pl.BlockSpec(memory_space=pltpu.VMEM)],
            out_specs=(pl.BlockSpec(memory_space=vmem), pl.BlockSpec(memory_space=vmem)),
            scratch_shapes=[
                vmem((steps + 1, BLOCKS, PITCH, CH), F32),
                vmem((2, TALL, SIDE, CH), F32),
                vmem((2, TALL, SIDE, CH), F32),
                vmem((steps, TALL, WIDE, CIN), BF16),
                vmem((steps, TALL, SIDE, CIN), BF16),
                vmem((steps, TALL, SIDE, CIN), BF16),
                vmem((2, BLOCKS * PITCH, CH), F32),
                vmem((3, 2, HALF, CIN), BF16),
                vmem((3, 2, HALF, CH), BF16),
                vmem((BLOCKS * PITCH, CH), F32),
                vmem((3, 2, HALF, CH), BF16),
                vmem((2, HALF, CH), F32),
                vmem((2, HALF, CIN), F32),
                vmem((PAIR, CIN), F32),
                vmem((9, CIN, 384), BF16),
                vmem((12 * CIN, CIN), BF16),
                vmem((9, CH, CIN), BF16),
                vmem((12 * CH, CIN), BF16),
                vmem((9, CH, CH), BF16),
                dma((4,)), dma((steps,)),
                dma((steps, SIDE)), dma((steps, SIDE)), dma((steps, SIDE)), dma((steps, SIDE)),
            ],
            compiler_params=pltpu.CompilerParams(collective_id=0, has_side_effects=True, vmem_limit_bytes=60 * 1024 * 1024),
        )(frames, h_init, w_x.reshape(9, CIN, 384), w_hzr.reshape(9, CH, CIN), w_hn.reshape(9, CH, CH), gate_bias)

    return jax.shard_map(local_fn, mesh=mesh, in_specs=(frame_spec, state_spec, P(), P(), P(), P()), out_specs=(frame_spec, state_spec), check_vma=False)
```

```python
import functools

import jax
import jax.numpy as jnp
from jax import lax
from jax.experimental import pallas as pl
from jax.experimental.pallas import tpu as pltpu
from jax.sharding import PartitionSpec as P

MESH = pl.DeviceIdType.MESH
F32 = jnp.float32
BF16 = jnp.bfloat16

CH, CIN, SIDE, EDGE, TALL, WIDE = 128, 256, 8, 16, 20, 64
PITCH = 80
BLOCKS = 22
CELLS = BLOCKS * PITCH
BLOCK = 3
OUTER = (1, 2, 19, 20)
DIRS = [(dr, dc) for dr in (-1, 0, 1) for dc in (-1, 0, 1) if (dr, dc) != (0, 0)]

MID = (32, WIDE)
LOW = (0, 32)
HIGH = (WIDE, PITCH)
ALL = (0, PITCH)
TIP = (0, EDGE)
GATE_CORE = [[(4, 11) + MID], [(11, 18) + MID]]
GATE_RIM = [[(2, 4) + ALL, (4, 7) + LOW], [(7, 15) + LOW], [(15, 18) + LOW, (4, 14) + HIGH],
            [(13, 18) + HIGH, (18, 20) + ALL, (20, 21) + TIP]]
CAND_CORE = [[(1, 4) + MID], [(4, 7) + MID]]
CAND_RIM = [[(0, 1) + ALL, (1, 6) + LOW], [(6, 7) + LOW, (1, 7) + HIGH, (7, 8) + ALL, (8, 9) + LOW]]
ZR_CORE = [(336, 272), (608, 272), (880, 288), (1168, 288)]
ZR_RIM = [(160, 176), (1440, 176)]
N_CORE = [[(2, 4) + ALL, (4, 5, 0, 48)], [(4, 5, 32, PITCH), (5, 7) + ALL]]
N_RIM = [[(0, 1) + ALL, (1, 2, 0, 48)], [(1, 2, 48, PITCH), (7, 8) + ALL, (8, 9) + TIP]]


def kernel(n_rows, n_cols, steps, frames, h_init, w_x, w_hzr, w_hn, bias, h_seq, h_last,
           hf, hl, hr, fs, fl, fr, xf, fx, ub, rh, vb, zb, gz, gn, wx, wxn, wh, whn, whr,
           sem_w, sem_f, f_send, f_recv, h_send, h_recv):
    row = lax.axis_index('rows')
    col = lax.axis_index('cols')

    def exists(dr, dc):
        conds = []
        if dr:
            conds.append(row + dr >= 0 if dr < 0 else row + dr < n_rows)
        if dc:
            conds.append(col + dc >= 0 if dc < 0 else col + dc < n_cols)
        return conds[0] if len(conds) == 1 else jnp.logical_and(*conds)

    def peer(dr, dc):
        return {'rows': lax.rem(row + dr + n_rows, n_rows), 'cols': lax.rem(col + dc + n_cols, n_cols)}

    def local_copies():
        return [pltpu.make_async_copy(w_x, wx, sem_w.at[0]), pltpu.make_async_copy(w_hzr, wh, sem_w.at[1]),
                pltpu.make_async_copy(w_hn, whr, sem_w.at[2]),
                pltpu.make_async_copy(h_init.at[0], hf.at[0, 3:19, EDGE:PITCH, :], sem_w.at[3])]

    def frame_copy(t):
        return pltpu.make_async_copy(frames.at[t, 0], fs.at[t, 2:18], sem_f.at[t])

    frame_copy(0).start()
    weights = local_copies()
    weights[3].start()
    weights[0].start()
    for t in range(1, BLOCK):
        frame_copy(t).start()
    weights[1].start()
    weights[2].start()

    barrier = pltpu.get_barrier_semaphore()
    count = jnp.int32(0)
    for d in DIRS:
        here = exists(*d)
        count = count + jnp.where(here, 1, 0)

        @pl.when(here)
        def _(d=d):
            pl.semaphore_signal(barrier, inc=1, device_id=peer(*d), device_id_type=MESH)
    pl.semaphore_wait(barrier, count)

    src_y = {-1: slice(0, 2), 0: slice(0, EDGE), 1: slice(14, EDGE)}
    dst_y = {-1: slice(18, TALL), 0: slice(2, 18), 1: slice(0, 2)}

    def frame_xfer(t, i, local=False):
        dr, dc = DIRS[i]
        cells, land = {0: (slice(0, WIDE), fs), -1: (slice(0, SIDE), fr), 1: (slice(WIDE - SIDE, WIDE), fl)}[dc]
        y = src_y[dr]
        src = fs.at[t, slice(y.start + 2, y.stop + 2), cells] if local else frames.at[t, 0, y, cells]
        return pltpu.make_async_remote_copy(src, land.at[t, dst_y[dr]], f_send.at[t, i], f_recv.at[t, i],
                                            device_id=peer(dr, dc), device_id_type=MESH)

    def state_xfer(t, i, slot):
        dr, dc = DIRS[i]
        k_src = {-1: 3, 0: 3, 1: 17}[dr]
        k_dst = {-1: 19, 0: 3, 1: 1}[dr]
        n = 2 if dr else EDGE
        if slot is None:
            flat = hf.at[t].reshape(BLOCKS * PITCH, CH)
            src = flat.at[pl.ds(PITCH * k_src + SIDE, 2 * PITCH)]
            dst = flat.at[pl.ds(PITCH * k_dst + SIDE, 2 * PITCH)]
        else:
            cells = {0: slice(EDGE, PITCH), -1: slice(EDGE, EDGE + SIDE), 1: slice(PITCH - SIDE, PITCH)}[dc]
            src = hf.at[t, slice(k_src, k_src + n), cells]
            dst = {0: hf.at[t, slice(k_dst, k_dst + n), cells], -1: hr.at[slot, dst_y[dr]], 1: hl.at[slot, dst_y[dr]]}[dc]
        return pltpu.make_async_remote_copy(src, dst, h_send.at[t, i], h_recv.at[t, i], device_id=peer(dr, dc), device_id_type=MESH)

    def start(make, rows_only=False):
        for i, d in enumerate(DIRS):
            if d[1] == 0 or not rows_only:
                @pl.when(exists(*d))
                def _(i=i):
                    make(i).start()

    def finish(make, rows_only=False):
        for i, (dr, dc) in enumerate(DIRS):
            if dc == 0 or not rows_only:
                @pl.when(exists(dr, dc))
                def _(i=i):
                    make(i).wait_send()

                @pl.when(exists(-dr, -dc))
                def _(i=i):
                    make(i).wait_recv()

    frame_copy(0).wait()
    start(lambda i: frame_xfer(0, i, True))
    weights[3].wait()
    start(lambda i: state_xfer(0, i, 0))

    def start_rest(t, carry):
        start(lambda i: frame_xfer(t, i))
        return carry

    lax.fori_loop(1, steps, start_rest, 0)
    for t in range(BLOCK, steps):
        frame_copy(t).start()

    for t in range(steps):
        hf[t, 0, 72:PITCH, :] = jnp.zeros((SIDE, CH), F32)
        hf[t, 1, 0:SIDE, :] = jnp.zeros((SIDE, CH), F32)
        hf[t, 21, SIDE:24, :] = jnp.zeros((EDGE, CH), F32)
    for slot in range(BLOCK):
        for half in range(2):
            xf[slot, half, 72:88, :] = jnp.zeros((EDGE, CH), F32)
            xf[slot, half, 21 * PITCH + SIDE:21 * PITCH + 24, :] = jnp.zeros((EDGE, CH), F32)

    @pl.when(row == 0)
    def _():
        for t in range(steps):
            hf[t, 1, SIDE:PITCH, :] = jnp.zeros((72, CH), F32)
            hf[t, 2, 0:PITCH, :] = jnp.zeros((PITCH, CH), F32)
            hf[t, 3, 0:SIDE, :] = jnp.zeros((SIDE, CH), F32)
            fs[t, 0:2] = jnp.zeros((2, WIDE, CIN), BF16)
            fl[t, 0:2] = jnp.zeros((2, SIDE, CIN), BF16)
            fr[t, 0:2] = jnp.zeros((2, SIDE, CIN), BF16)
        for s in range(2):
            hl[s, 0:2] = jnp.zeros((2, SIDE, CH), F32)
            hr[s, 0:2] = jnp.zeros((2, SIDE, CH), F32)

    @pl.when(row == n_rows - 1)
    def _():
        for t in range(steps):
            hf[t, 19, SIDE:PITCH, :] = jnp.zeros((72, CH), F32)
            hf[t, TALL, 0:PITCH, :] = jnp.zeros((PITCH, CH), F32)
            hf[t, 21, 0:SIDE, :] = jnp.zeros((SIDE, CH), F32)
            fs[t, 18:TALL] = jnp.zeros((2, WIDE, CIN), BF16)
            fl[t, 18:TALL] = jnp.zeros((2, SIDE, CIN), BF16)
            fr[t, 18:TALL] = jnp.zeros((2, SIDE, CIN), BF16)
        for s in range(2):
            hl[s, 18:TALL] = jnp.zeros((2, SIDE, CH), F32)
            hr[s, 18:TALL] = jnp.zeros((2, SIDE, CH), F32)

    @pl.when(col == 0)
    def _():
        for t in range(steps):
            fl[t] = jnp.zeros((TALL, SIDE, CIN), BF16)
        hl[...] = jnp.zeros((2, TALL, SIDE, CH), F32)

    @pl.when(col == n_cols - 1)
    def _():
        for t in range(steps):
            fr[t] = jnp.zeros((TALL, SIDE, CIN), BF16)
        hr[...] = jnp.zeros((2, TALL, SIDE, CH), F32)

    for c in range(3):
        vb[c, 1616:1696, :] = jnp.zeros((PITCH, CH), BF16)
    rh[2 * PITCH - SIDE:2 * PITCH, :] = jnp.zeros((SIDE, CH), F32)
    rh[TALL * PITCH + EDGE:TALL * PITCH + 24, :] = jnp.zeros((SIDE, CH), F32)

    def two_rows(dst, src, depth, lanes):
        zero = jnp.zeros((depth, CH), BF16)
        for c in range(3):
            for a in range(4):
                i = (a * 3 + c) * depth
                dst[i:i + depth, 0:CH] = src[a * 3 + c, :, lanes] if a < 3 else zero
                dst[i:i + depth, CH:2 * CH] = src[a * 3 + c - 3, :, lanes] if a > 0 else zero

    weights[0].wait()
    two_rows(wxn, wx, CIN, slice(2 * CH, 3 * CH))

    def take(ref, boxes):
        parts = [ref[k0:k1, j0:j1, :] for k0, k1, j0, j1 in boxes]
        return jnp.concatenate([x.reshape(-1, x.shape[-1]) for x in parts], axis=0)

    def put(ref, boxes, value):
        at = 0
        for k0, k1, j0, j1 in boxes:
            size = (k1 - k0) * (j1 - j0)
            ref[k0:k1, j0:j1, :] = value[at:at + size].reshape(k1 - k0, j1 - j0, value.shape[-1])
            at += size

    def two_row_patches(ref, depth, boxes):
        taps = []
        for a in range(4):
            lead = 1 + a // 2
            for c in range(3):
                rows = ref.at[c].reshape(BLOCKS // 2, 2, PITCH, depth)
                parts = [rows[y0 + lead:y1 + lead, a % 2, j0:j1, :] for y0, y1, j0, j1 in boxes]
                taps.append(jnp.concatenate([x.reshape(-1, depth) for x in parts], axis=0))
        return jnp.concatenate(taps, axis=1)

    def matmul(lhs, w):
        return jnp.dot(lhs, w, preferred_element_type=F32)

    def shifted(dst, src, lo, hi):
        for c in range(3):
            dst[c, lo:hi, :] = src[lo - 1 + c:hi - 1 + c, :].astype(BF16)

    halves = [(half, slice(half * CH, half * CH + CH)) for half in range(2)]

    def prep_core(t, slot):
        for half, lanes in halves:
            cells = xf.at[slot, half].reshape(BLOCKS, PITCH, CH)
            cells[3:19, EDGE:PITCH, :] = fs[t, 2:18, :, lanes].astype(F32)
            for c in range(3):
                fx[slot, c, 3:19, 32:WIDE, lanes] = cells[3:19, 31 + c:63 + c, :].astype(BF16)

    def prep_rim(t, slot):
        for half, lanes in halves:
            flat = xf.at[slot, half]
            cells = flat.reshape(BLOCKS, PITCH, CH)
            cells[1:3, EDGE:PITCH, :] = fs[t, 0:2, :, lanes].astype(F32)
            cells[19:21, EDGE:PITCH, :] = fs[t, 18:TALL, :, lanes].astype(F32)
            cells[1:21, SIDE:EDGE, :] = fl[t, :, :, lanes].astype(F32)
            cells[2:22, 0:SIDE, :] = fr[t, :, :, lanes].astype(F32)
            for c in range(3):
                out = fx.at[slot, c]
                for k in OUTER:
                    first = PITCH * k - 1 + c
                    out[k, :, lanes] = flat[first:first + PITCH, :].astype(BF16)
                out[21, 0:EDGE, lanes] = flat[PITCH * 21 - 1 + c:PITCH * 21 - 1 + c + EDGE, :].astype(BF16)
                for k in range(3, 19):
                    first = PITCH * k - 1 + c
                    out[k, 0:32, lanes] = flat[first:first + 32, :].astype(BF16)
                    out[k, WIDE:PITCH, lanes] = flat[first + WIDE:first + PITCH, :].astype(BF16)

    def gates(slot, chunks):
        bias_zr = bias[0:2 * CH][None, :]
        wzr = wx[:, :, 0:2 * CH].reshape(9 * CIN, 2 * CH)
        for boxes in chunks:
            taps = [take(fx.at[slot, c], [(k0 + a, k1 + a, j0, j1) for k0, k1, j0, j1 in boxes]) for a in (-1, 0, 1) for c in range(3)]
            put(gz.at[slot], boxes, matmul(jnp.concatenate(taps, axis=1), wzr) + bias_zr)

    def cand_gates(slot, chunks):
        bias_n = bias[2 * CH:3 * CH]
        bias_n = jnp.concatenate([bias_n, bias_n])[None, :]
        for boxes in chunks:
            put(gn.at[slot], boxes, matmul(two_row_patches(fx.at[slot], CIN, boxes), wxn[...]) + bias_n)

    def zr_gates(slot, h_flat, chunks):
        whzr = wh[...].reshape(9 * CH, 2 * CH)
        base = gz.at[slot].reshape(CELLS, 2 * CH)
        for lo, size in chunks:
            here = slice(lo, lo + size)
            taps = [ub[c, lo + a:lo + a + size, :] for a in (-PITCH, 0, PITCH) for c in range(3)]
            gate = 0.5 * jnp.tanh(0.5 * (matmul(jnp.concatenate(taps, axis=1), whzr) + base[here, :])) + 0.5
            zb[here, :] = gate[:, 0:CH]
            rh[here, :] = gate[:, CH:2 * CH] * h_flat[here, :]

    left_edge = col == 0
    right_edge = col == n_cols - 1

    def new_state(t, slot, chunks):
        def rows_of(ref, n):
            return ref.reshape(n // 2, 2, ref.shape[-2], CH)
        old, new = rows_of(hf.at[t].reshape(BLOCKS, PITCH, CH), BLOCKS), rows_of(hf.at[t + 1].reshape(BLOCKS, PITCH, CH), BLOCKS)
        update = zb.reshape(BLOCKS // 2, 2, PITCH, CH)
        seq, final = rows_of(h_seq.at[t, 0], EDGE), rows_of(h_last.at[0], EDGE)
        for boxes in chunks:
            cand = jnp.tanh(matmul(two_row_patches(vb, CH, boxes), whn[...]) + take(gn.at[slot], boxes))
            at = 0
            for y0, y1, j0, j1 in boxes:
                n = (y1 - y0) * (j1 - j0)
                for odd in range(2):
                    if y0 == SIDE and odd:
                        continue
                    ks = slice(y0 + 1 + odd, y1 + 1 + odd)
                    par = 1 - odd
                    z = update[ks, par, j0:j1, :]
                    c = cand[at:at + n, odd * CH:odd * CH + CH].reshape(y1 - y0, j1 - j0, CH)
                    h_new = (1.0 - z) * c + z * old[ks, par, j0:j1, :]
                    lo = max(j0, EDGE)
                    if lo < j1:
                        main = h_new[:, lo - j0:]
                        seq[y0:y1, odd, lo - EDGE:j1 - EDGE, :] = main.astype(BF16)
                        final[y0:y1, odd, lo - EDGE:j1 - EDGE, :] = main
                        new[ks, par, lo:j1, :] = main
                    if j0 == 0 and y0 < SIDE:
                        new[ks, par, SIDE:EDGE, :] = jnp.where(left_edge, 0.0, h_new[:, SIDE:EDGE])
                    if j0 == 0 and (y0 or odd):
                        new[ks, par, 0:SIDE, :] = jnp.where(right_edge, 0.0, h_new[:, 0:SIDE])
                at += n

    def block(b, carry):
        t0 = b * BLOCK

        @pl.when(b == 0)
        def _():
            for t in range(1, BLOCK):
                frame_copy(t).wait()

        @pl.when(b > 0)
        def _():
            for j in range(BLOCK):
                frame_copy(t0 + j).wait()

        for j in range(BLOCK):
            prep_core(t0 + j, j)
            gates(j, GATE_CORE)
        for j in range(BLOCK - 1):
            cand_gates(j, [CAND_CORE[0] + CAND_CORE[1]])
        cand_gates(BLOCK - 1, CAND_CORE)

        @pl.when(b == 0)
        def _():
            weights[1].wait()
            weights[2].wait()
            two_rows(whn, whr, CH, slice(0, CH))

        finish(lambda i: frame_xfer(t0, i))
        prep_rim(t0, 0)
        gates(0, GATE_RIM)
        cand_gates(0, CAND_RIM)
        finish(lambda i: state_xfer(t0, i, b))
        hf[t0, 1:21, SIDE:EDGE, :] = hl[b]
        hf[t0, 2:22, 0:SIDE, :] = hr[b]
        h_flat = hf.at[t0].reshape(CELLS, CH)
        shifted(ub, h_flat, PITCH, 1696)
        zr_gates(0, h_flat, ZR_CORE + ZR_RIM)
        shifted(vb, rh, 160, 1616)
        new_state(t0, 0, N_CORE + N_RIM)
        start(lambda i: state_xfer(t0 + 1, i, None), True)

        for j in range(1, BLOCK):
            t = t0 + j
            finish(lambda i: frame_xfer(t, i))
            h_flat = hf.at[t].reshape(CELLS, CH)
            prep_rim(t, j)
            shifted(ub, h_flat, 256, 1520)
            ends = h_flat[1520:1528, :]
            for c, x in enumerate((h_flat[1519:1527, :], ends, pltpu.roll(ends, SIDE - 1, 0))):
                ub[c, 1520:1528, :] = x.astype(BF16)
            gates(j, GATE_RIM)
            zr_gates(j, h_flat, ZR_CORE)
            shifted(vb, rh, 480, 1440)
            cand_gates(j, CAND_RIM)
            new_state(t, j, N_CORE)
            finish(lambda i: state_xfer(t, i, None), True)
            shifted(ub, h_flat, PITCH, 256)
            shifted(ub, h_flat, 1520, 1696)
            zr_gates(j, h_flat, ZR_RIM)
            shifted(vb, rh, 160, 480)
            shifted(vb, rh, 1440, 1616)
            new_state(t, j, N_RIM)
            if j < BLOCK - 1:
                start(lambda i: state_xfer(t + 1, i, None), True)
            else:
                @pl.when(b == 0)
                def _():
                    start(lambda i: state_xfer(t + 1, i, 1))
        return carry

    lax.fori_loop(0, steps // BLOCK, block, 0)


def solution(mesh):
    n_rows = mesh.shape['rows']
    n_cols = mesh.shape['cols']
    frame_spec = P(None, 'batch', 'rows', 'cols', None)
    state_spec = P('batch', 'rows', 'cols', None)

    def local_fn(frames, h_init, w_x, w_hzr, w_hn, gate_bias):
        steps = frames.shape[0]
        any_spec = pl.BlockSpec(memory_space=pl.ANY)
        vmem = pltpu.VMEM
        dma = pltpu.SemaphoreType.DMA
        return pl.pallas_call(
            functools.partial(kernel, n_rows, n_cols, steps),
            out_shape=(vmem((steps, 1, EDGE, WIDE, CH), BF16), vmem((1, EDGE, WIDE, CH), F32)),
            in_specs=[any_spec] * 5 + [pl.BlockSpec(memory_space=pltpu.VMEM)],
            out_specs=(pl.BlockSpec(memory_space=vmem), pl.BlockSpec(memory_space=vmem)),
            scratch_shapes=[
                vmem((steps + 1, BLOCKS, PITCH, CH), F32),
                vmem((2, TALL, SIDE, CH), F32),
                vmem((2, TALL, SIDE, CH), F32),
                vmem((steps, TALL, WIDE, CIN), BF16),
                vmem((steps, TALL, SIDE, CIN), BF16),
                vmem((steps, TALL, SIDE, CIN), BF16),
                vmem((BLOCK, 2, BLOCKS * PITCH, CH), F32),
                vmem((BLOCK, 3, BLOCKS, PITCH, CIN), BF16),
                vmem((3, CELLS, CH), BF16),
                vmem((BLOCKS * PITCH, CH), F32),
                vmem((3, CELLS, CH), BF16),
                vmem((CELLS, CH), F32),
                vmem((BLOCK, BLOCKS, PITCH, CIN), F32),
                vmem((BLOCK, 9, PITCH, CIN), F32),
                vmem((9, CIN, 384), BF16),
                vmem((12 * CIN, CIN), BF16),
                vmem((9, CH, CIN), BF16),
                vmem((12 * CH, CIN), BF16),
                vmem((9, CH, CH), BF16),
                dma((4,)), dma((steps,)),
                dma((steps, SIDE)), dma((steps, SIDE)), dma((steps, SIDE)), dma((steps, SIDE)),
            ],
            compiler_params=pltpu.CompilerParams(collective_id=0, has_side_effects=True, vmem_limit_bytes=60 * 1024 * 1024),
        )(frames, h_init, w_x.reshape(9, CIN, 384), w_hzr.reshape(9, CH, CIN), w_hn.reshape(9, CH, CH), gate_bias)

    return jax.shard_map(local_fn, mesh=mesh, in_specs=(frame_spec, state_spec, P(), P(), P(), P()), out_specs=(frame_spec, state_spec), check_vma=False)
```

```python
import functools

import jax
import jax.numpy as jnp
from jax import lax
from jax.experimental import pallas as pl
from jax.experimental.pallas import tpu as pltpu
from jax.sharding import PartitionSpec as P

MESH = pl.DeviceIdType.MESH
F32 = jnp.float32
BF16 = jnp.bfloat16

CH, CIN, SIDE, EDGE, TALL, WIDE = 128, 256, 8, 16, 20, 64
PITCH = 80
BLOCKS = 22
CELLS = BLOCKS * PITCH
BLOCK = 3
OUTER = (1, 2, 19, 20)
DIRS = [(dr, dc) for dr in (-1, 0, 1) for dc in (-1, 0, 1) if (dr, dc) != (0, 0)]

MID = (32, WIDE)
LOW = (0, 32)
HIGH = (WIDE, PITCH)
ALL = (0, PITCH)
TIP = (0, EDGE)
GATE_CORE = [[(4, 11) + MID], [(11, 18) + MID]]
GATE_RIM = [[(2, 4) + ALL, (4, 7) + LOW], [(7, 15) + LOW], [(15, 18) + LOW, (4, 14) + HIGH],
            [(13, 18) + HIGH, (18, 20) + ALL, (20, 21) + TIP]]
CAND_CORE = [[(1, 4) + MID], [(4, 7) + MID]]
CAND_RIM = [[(0, 1) + ALL, (1, 6) + LOW], [(6, 7) + LOW, (1, 7) + HIGH, (7, 8) + ALL, (8, 9) + LOW]]
ZR_CORE = [(336, 272), (608, 272), (880, 288), (1168, 288)]
ZR_RIM = [(160, 176), (1440, 176)]
N_CORE = [[(2, 4) + ALL, (4, 5, 0, 48)], [(4, 5, 32, PITCH), (5, 7) + ALL]]
N_RIM = [[(0, 1) + ALL, (1, 2, 0, 48)], [(1, 2, 48, PITCH), (7, 8) + ALL, (8, 9) + TIP]]


def kernel(n_rows, n_cols, steps, frames, h_init, w_x, w_hzr, w_hn, bias, h_seq, h_last,
           hf, hl, hr, fs, fl, fr, xf, fx, ub, rh, vb, zb, gz, gn, wx, wxn, wh, whn, whr,
           sem_w, sem_f, f_send, f_recv, h_send, h_recv):
    row = lax.axis_index('rows')
    col = lax.axis_index('cols')

    def exists(dr, dc):
        conds = []
        if dr:
            conds.append(row + dr >= 0 if dr < 0 else row + dr < n_rows)
        if dc:
            conds.append(col + dc >= 0 if dc < 0 else col + dc < n_cols)
        return conds[0] if len(conds) == 1 else jnp.logical_and(*conds)

    def peer(dr, dc):
        return {'rows': lax.rem(row + dr + n_rows, n_rows), 'cols': lax.rem(col + dc + n_cols, n_cols)}

    def local_copies():
        return [pltpu.make_async_copy(w_x, wx, sem_w.at[0]), pltpu.make_async_copy(w_hzr, wh, sem_w.at[1]),
                pltpu.make_async_copy(w_hn, whr, sem_w.at[2]),
                pltpu.make_async_copy(h_init.at[0], hf.at[0, 3:19, EDGE:PITCH, :], sem_w.at[3])]

    def frame_copy(t):
        return pltpu.make_async_copy(frames.at[t, 0], fs.at[t, 2:18], sem_f.at[t])

    frame_copy(0).start()
    weights = local_copies()
    weights[3].start()
    weights[0].start()
    for t in range(1, BLOCK):
        frame_copy(t).start()
    weights[1].start()
    weights[2].start()

    barrier = pltpu.get_barrier_semaphore()
    count = jnp.int32(0)
    for d in DIRS:
        here = exists(*d)
        count = count + jnp.where(here, 1, 0)

        @pl.when(here)
        def _(d=d):
            pl.semaphore_signal(barrier, inc=1, device_id=peer(*d), device_id_type=MESH)
    pl.semaphore_wait(barrier, count)

    src_y = {-1: slice(0, 2), 0: slice(0, EDGE), 1: slice(14, EDGE)}
    dst_y = {-1: slice(18, TALL), 0: slice(2, 18), 1: slice(0, 2)}

    def frame_xfer(t, i, local=False):
        dr, dc = DIRS[i]
        cells, land = {0: (slice(0, WIDE), fs), -1: (slice(0, SIDE), fr), 1: (slice(WIDE - SIDE, WIDE), fl)}[dc]
        y = src_y[dr]
        src = fs.at[t, slice(y.start + 2, y.stop + 2), cells] if local else frames.at[t, 0, y, cells]
        return pltpu.make_async_remote_copy(src, land.at[t, dst_y[dr]], f_send.at[t, i], f_recv.at[t, i],
                                            device_id=peer(dr, dc), device_id_type=MESH)

    def state_xfer(t, i, slot):
        dr, dc = DIRS[i]
        k_src = {-1: 3, 0: 3, 1: 17}[dr]
        k_dst = {-1: 19, 0: 3, 1: 1}[dr]
        n = 2 if dr else EDGE
        if slot is None:
            flat = hf.at[t].reshape(BLOCKS * PITCH, CH)
            src = flat.at[pl.ds(PITCH * k_src + SIDE, 2 * PITCH)]
            dst = flat.at[pl.ds(PITCH * k_dst + SIDE, 2 * PITCH)]
        else:
            cells = {0: slice(EDGE, PITCH), -1: slice(EDGE, EDGE + SIDE), 1: slice(PITCH - SIDE, PITCH)}[dc]
            src = hf.at[t, slice(k_src, k_src + n), cells]
            dst = {0: hf.at[t, slice(k_dst, k_dst + n), cells], -1: hr.at[slot, dst_y[dr]], 1: hl.at[slot, dst_y[dr]]}[dc]
        return pltpu.make_async_remote_copy(src, dst, h_send.at[t, i], h_recv.at[t, i], device_id=peer(dr, dc), device_id_type=MESH)

    def start(make, rows_only=False):
        for i, d in enumerate(DIRS):
            if d[1] == 0 or not rows_only:
                @pl.when(exists(*d))
                def _(i=i):
                    make(i).start()

    def finish(make, rows_only=False):
        for i, (dr, dc) in enumerate(DIRS):
            if dc == 0 or not rows_only:
                @pl.when(exists(dr, dc))
                def _(i=i):
                    make(i).wait_send()

                @pl.when(exists(-dr, -dc))
                def _(i=i):
                    make(i).wait_recv()

    frame_copy(0).wait()
    start(lambda i: frame_xfer(0, i, True))
    weights[3].wait()
    start(lambda i: state_xfer(0, i, 0))

    def start_rest(t, carry):
        start(lambda i: frame_xfer(t, i))
        return carry

    lax.fori_loop(1, steps, start_rest, 0)
    for t in range(BLOCK, steps):
        frame_copy(t).start()

    for t in range(steps):
        hf[t, 0, 72:PITCH, :] = jnp.zeros((SIDE, CH), F32)
        hf[t, 1, 0:SIDE, :] = jnp.zeros((SIDE, CH), F32)
        hf[t, 21, SIDE:24, :] = jnp.zeros((EDGE, CH), F32)
    for slot in range(BLOCK):
        for half in range(2):
            xf[slot, half, 72:88, :] = jnp.zeros((EDGE, CH), F32)
            xf[slot, half, 21 * PITCH + SIDE:21 * PITCH + 24, :] = jnp.zeros((EDGE, CH), F32)

    @pl.when(row == 0)
    def _():
        for t in range(steps):
            hf[t, 1, SIDE:PITCH, :] = jnp.zeros((72, CH), F32)
            hf[t, 2, 0:PITCH, :] = jnp.zeros((PITCH, CH), F32)
            hf[t, 3, 0:SIDE, :] = jnp.zeros((SIDE, CH), F32)
            fs[t, 0:2] = jnp.zeros((2, WIDE, CIN), BF16)
            fl[t, 0:2] = jnp.zeros((2, SIDE, CIN), BF16)
            fr[t, 0:2] = jnp.zeros((2, SIDE, CIN), BF16)
        for s in range(2):
            hl[s, 0:2] = jnp.zeros((2, SIDE, CH), F32)
            hr[s, 0:2] = jnp.zeros((2, SIDE, CH), F32)

    @pl.when(row == n_rows - 1)
    def _():
        for t in range(steps):
            hf[t, 19, SIDE:PITCH, :] = jnp.zeros((72, CH), F32)
            hf[t, TALL, 0:PITCH, :] = jnp.zeros((PITCH, CH), F32)
            hf[t, 21, 0:SIDE, :] = jnp.zeros((SIDE, CH), F32)
            fs[t, 18:TALL] = jnp.zeros((2, WIDE, CIN), BF16)
            fl[t, 18:TALL] = jnp.zeros((2, SIDE, CIN), BF16)
            fr[t, 18:TALL] = jnp.zeros((2, SIDE, CIN), BF16)
        for s in range(2):
            hl[s, 18:TALL] = jnp.zeros((2, SIDE, CH), F32)
            hr[s, 18:TALL] = jnp.zeros((2, SIDE, CH), F32)

    @pl.when(col == 0)
    def _():
        for t in range(steps):
            fl[t] = jnp.zeros((TALL, SIDE, CIN), BF16)
        hl[...] = jnp.zeros((2, TALL, SIDE, CH), F32)

    @pl.when(col == n_cols - 1)
    def _():
        for t in range(steps):
            fr[t] = jnp.zeros((TALL, SIDE, CIN), BF16)
        hr[...] = jnp.zeros((2, TALL, SIDE, CH), F32)

    for c in range(3):
        vb[c, 1616:1696, :] = jnp.zeros((PITCH, CH), BF16)
    rh[2 * PITCH - SIDE:2 * PITCH, :] = jnp.zeros((SIDE, CH), F32)
    rh[TALL * PITCH + EDGE:TALL * PITCH + 24, :] = jnp.zeros((SIDE, CH), F32)

    def two_rows(dst, src, depth, lanes):
        zero = jnp.zeros((depth, CH), BF16)
        for c in range(3):
            for a in range(4):
                i = (a * 3 + c) * depth
                dst[i:i + depth, 0:CH] = src[a * 3 + c, :, lanes] if a < 3 else zero
                dst[i:i + depth, CH:2 * CH] = src[a * 3 + c - 3, :, lanes] if a > 0 else zero

    weights[0].wait()
    two_rows(wxn, wx, CIN, slice(2 * CH, 3 * CH))

    def take(ref, boxes):
        parts = [ref[k0:k1, j0:j1, :] for k0, k1, j0, j1 in boxes]
        return jnp.concatenate([x.reshape(-1, x.shape[-1]) for x in parts], axis=0)

    def put(ref, boxes, value):
        at = 0
        for k0, k1, j0, j1 in boxes:
            size = (k1 - k0) * (j1 - j0)
            ref[k0:k1, j0:j1, :] = value[at:at + size].reshape(k1 - k0, j1 - j0, value.shape[-1])
            at += size

    def two_row_patches(ref, depth, boxes):
        taps = []
        for a in range(4):
            lead = 1 + a // 2
            for c in range(3):
                rows = ref.at[c].reshape(BLOCKS // 2, 2, PITCH, depth)
                parts = [rows[y0 + lead:y1 + lead, a % 2, j0:j1, :] for y0, y1, j0, j1 in boxes]
                taps.append(jnp.concatenate([x.reshape(-1, depth) for x in parts], axis=0))
        return jnp.concatenate(taps, axis=1)

    def matmul(lhs, w):
        return jnp.dot(lhs, w, preferred_element_type=F32)

    def shifted(dst, src, lo, hi):
        for c in range(3):
            dst[c, lo:hi, :] = src[lo - 1 + c:hi - 1 + c, :].astype(BF16)

    halves = [(half, slice(half * CH, half * CH + CH)) for half in range(2)]

    def prep_core(t, slot):
        for half, lanes in halves:
            cells = xf.at[slot, half].reshape(BLOCKS, PITCH, CH)
            cells[3:19, EDGE:PITCH, :] = fs[t, 2:18, :, lanes].astype(F32)
            for c in range(3):
                fx[slot, c, 3:19, 32:WIDE, lanes] = cells[3:19, 31 + c:63 + c, :].astype(BF16)

    def prep_rim(t, slot):
        for half, lanes in halves:
            flat = xf.at[slot, half]
            cells = flat.reshape(BLOCKS, PITCH, CH)
            cells[1:3, EDGE:PITCH, :] = fs[t, 0:2, :, lanes].astype(F32)
            cells[19:21, EDGE:PITCH, :] = fs[t, 18:TALL, :, lanes].astype(F32)
            cells[1:21, SIDE:EDGE, :] = fl[t, :, :, lanes].astype(F32)
            cells[2:22, 0:SIDE, :] = fr[t, :, :, lanes].astype(F32)
            for c in range(3):
                out = fx.at[slot, c]
                for k in OUTER:
                    first = PITCH * k - 1 + c
                    out[k, :, lanes] = flat[first:first + PITCH, :].astype(BF16)
                out[21, 0:EDGE, lanes] = flat[PITCH * 21 - 1 + c:PITCH * 21 - 1 + c + EDGE, :].astype(BF16)
                for k in range(3, 19):
                    first = PITCH * k - 1 + c
                    out[k, 0:32, lanes] = flat[first:first + 32, :].astype(BF16)
                    out[k, WIDE:PITCH, lanes] = flat[first + WIDE:first + PITCH, :].astype(BF16)

    def gates(slot, chunks):
        bias_zr = bias[0:2 * CH][None, :]
        wzr = wx[:, :, 0:2 * CH].reshape(9 * CIN, 2 * CH)
        for boxes in chunks:
            taps = [take(fx.at[slot, c], [(k0 + a, k1 + a, j0, j1) for k0, k1, j0, j1 in boxes]) for a in (-1, 0, 1) for c in range(3)]
            put(gz.at[slot], boxes, matmul(jnp.concatenate(taps, axis=1), wzr) + bias_zr)

    def cand_gates(slot, chunks):
        bias_n = bias[2 * CH:3 * CH]
        bias_n = jnp.concatenate([bias_n, bias_n])[None, :]
        for boxes in chunks:
            put(gn.at[slot], boxes, matmul(two_row_patches(fx.at[slot], CIN, boxes), wxn[...]) + bias_n)

    def zr_gates(slot, h_flat, chunks):
        whzr = wh[...].reshape(9 * CH, 2 * CH)
        base = gz.at[slot].reshape(CELLS, 2 * CH)
        for lo, size in chunks:
            here = slice(lo, lo + size)
            taps = [ub[c, lo + a:lo + a + size, :] for a in (-PITCH, 0, PITCH) for c in range(3)]
            gate = 0.5 * jnp.tanh(0.5 * (matmul(jnp.concatenate(taps, axis=1), whzr) + base[here, :])) + 0.5
            zb[here, :] = gate[:, 0:CH]
            rh[here, :] = gate[:, CH:2 * CH] * h_flat[here, :]

    left_edge = col == 0
    right_edge = col == n_cols - 1

    def new_state(t, slot, chunks):
        def rows_of(ref, n):
            return ref.reshape(n // 2, 2, ref.shape[-2], CH)
        old, new = rows_of(hf.at[t].reshape(BLOCKS, PITCH, CH), BLOCKS), rows_of(hf.at[t + 1].reshape(BLOCKS, PITCH, CH), BLOCKS)
        update = zb.reshape(BLOCKS // 2, 2, PITCH, CH)
        seq, final = rows_of(h_seq.at[t, 0], EDGE), rows_of(h_last.at[0], EDGE)
        for boxes in chunks:
            cand = jnp.tanh(matmul(two_row_patches(vb, CH, boxes), whn[...]) + take(gn.at[slot], boxes))
            at = 0
            for y0, y1, j0, j1 in boxes:
                n = (y1 - y0) * (j1 - j0)
                for odd in range(2):
                    if y0 == SIDE and odd:
                        continue
                    ks = slice(y0 + 1 + odd, y1 + 1 + odd)
                    par = 1 - odd
                    z = update[ks, par, j0:j1, :]
                    c = cand[at:at + n, odd * CH:odd * CH + CH].reshape(y1 - y0, j1 - j0, CH)
                    h_new = (1.0 - z) * c + z * old[ks, par, j0:j1, :]
                    lo = max(j0, EDGE)
                    if lo < j1:
                        main = h_new[:, lo - j0:]
                        seq[y0:y1, odd, lo - EDGE:j1 - EDGE, :] = main.astype(BF16)
                        final[y0:y1, odd, lo - EDGE:j1 - EDGE, :] = main
                        new[ks, par, lo:j1, :] = main
                    if j0 == 0 and y0 < SIDE:
                        new[ks, par, SIDE:EDGE, :] = jnp.where(left_edge, 0.0, h_new[:, SIDE:EDGE])
                    if j0 == 0 and (y0 or odd):
                        new[ks, par, 0:SIDE, :] = jnp.where(right_edge, 0.0, h_new[:, 0:SIDE])
                at += n

    def block(b, carry):
        t0 = b * BLOCK

        @pl.when(b == 0)
        def _():
            for t in range(1, BLOCK):
                frame_copy(t).wait()

        @pl.when(b > 0)
        def _():
            for j in range(BLOCK):
                frame_copy(t0 + j).wait()

        for j in range(BLOCK):
            prep_core(t0 + j, j)
            gates(j, GATE_CORE)
        for j in range(BLOCK - 1):
            cand_gates(j, [CAND_CORE[0] + CAND_CORE[1]])
        cand_gates(BLOCK - 1, CAND_CORE)

        @pl.when(b == 0)
        def _():
            weights[1].wait()
            weights[2].wait()
            two_rows(whn, whr, CH, slice(0, CH))

        finish(lambda i: frame_xfer(t0, i))
        prep_rim(t0, 0)
        gates(0, GATE_RIM)
        cand_gates(0, CAND_RIM)
        finish(lambda i: state_xfer(t0, i, b))
        hf[t0, 1:21, SIDE:EDGE, :] = hl[b]
        hf[t0, 2:22, 0:SIDE, :] = hr[b]
        h_flat = hf.at[t0].reshape(CELLS, CH)
        shifted(ub, h_flat, PITCH, 1696)
        zr_gates(0, h_flat, ZR_CORE + ZR_RIM)
        shifted(vb, rh, 160, 1616)
        new_state(t0, 0, N_CORE + N_RIM)
        start(lambda i: state_xfer(t0 + 1, i, None), True)

        for j in range(1, BLOCK):
            t = t0 + j
            finish(lambda i: frame_xfer(t, i))
            h_flat = hf.at[t].reshape(CELLS, CH)
            prep_rim(t, j)
            shifted(ub, h_flat, 256, 1520)
            ends = h_flat[1520:1528, :]
            for c, x in enumerate((h_flat[1519:1527, :], ends, pltpu.roll(ends, SIDE - 1, 0))):
                ub[c, 1520:1528, :] = x.astype(BF16)
            gates(j, GATE_RIM)
            zr_gates(j, h_flat, ZR_CORE)
            shifted(vb, rh, 480, 1440)
            cand_gates(j, CAND_RIM)
            finish(lambda i: state_xfer(t, i, None), True)
            shifted(ub, h_flat, PITCH, 256)
            shifted(ub, h_flat, 1520, 1696)
            zr_gates(j, h_flat, ZR_RIM)
            new_state(t, j, N_CORE[::-1])
            shifted(vb, rh, 160, 480)
            shifted(vb, rh, 1440, 1616)
            new_state(t, j, N_RIM)
            if j < BLOCK - 1:
                start(lambda i: state_xfer(t + 1, i, None), True)
            else:
                @pl.when(b == 0)
                def _():
                    start(lambda i: state_xfer(t + 1, i, 1))
        return carry

    lax.fori_loop(0, steps // BLOCK, block, 0)


def solution(mesh):
    n_rows = mesh.shape['rows']
    n_cols = mesh.shape['cols']
    frame_spec = P(None, 'batch', 'rows', 'cols', None)
    state_spec = P('batch', 'rows', 'cols', None)

    def local_fn(frames, h_init, w_x, w_hzr, w_hn, gate_bias):
        steps = frames.shape[0]
        any_spec = pl.BlockSpec(memory_space=pl.ANY)
        vmem = pltpu.VMEM
        dma = pltpu.SemaphoreType.DMA
        return pl.pallas_call(
            functools.partial(kernel, n_rows, n_cols, steps),
            out_shape=(vmem((steps, 1, EDGE, WIDE, CH), BF16), vmem((1, EDGE, WIDE, CH), F32)),
            in_specs=[any_spec] * 5 + [pl.BlockSpec(memory_space=pltpu.VMEM)],
            out_specs=(pl.BlockSpec(memory_space=vmem), pl.BlockSpec(memory_space=vmem)),
            scratch_shapes=[
                vmem((steps + 1, BLOCKS, PITCH, CH), F32),
                vmem((2, TALL, SIDE, CH), F32),
                vmem((2, TALL, SIDE, CH), F32),
                vmem((steps, TALL, WIDE, CIN), BF16),
                vmem((steps, TALL, SIDE, CIN), BF16),
                vmem((steps, TALL, SIDE, CIN), BF16),
                vmem((BLOCK, 2, BLOCKS * PITCH, CH), F32),
                vmem((BLOCK, 3, BLOCKS, PITCH, CIN), BF16),
                vmem((3, CELLS, CH), BF16),
                vmem((BLOCKS * PITCH, CH), F32),
                vmem((3, CELLS, CH), BF16),
                vmem((CELLS, CH), F32),
                vmem((BLOCK, BLOCKS, PITCH, CIN), F32),
                vmem((BLOCK, 9, PITCH, CIN), F32),
                vmem((9, CIN, 384), BF16),
                vmem((12 * CIN, CIN), BF16),
                vmem((9, CH, CIN), BF16),
                vmem((12 * CH, CIN), BF16),
                vmem((9, CH, CH), BF16),
                dma((4,)), dma((steps,)),
                dma((steps, SIDE)), dma((steps, SIDE)), dma((steps, SIDE)), dma((steps, SIDE)),
            ],
            compiler_params=pltpu.CompilerParams(collective_id=0, has_side_effects=True, vmem_limit_bytes=60 * 1024 * 1024),
        )(frames, h_init, w_x.reshape(9, CIN, 384), w_hzr.reshape(9, CH, CIN), w_hn.reshape(9, CH, CH), gate_bias)

    return jax.shard_map(local_fn, mesh=mesh, in_specs=(frame_spec, state_spec, P(), P(), P(), P()), out_specs=(frame_spec, state_spec), check_vma=False)
```

```python
import functools

import jax
import jax.numpy as jnp
from jax import lax
from jax.experimental import pallas as pl
from jax.experimental.pallas import tpu as pltpu
from jax.sharding import PartitionSpec as P

MESH = pl.DeviceIdType.MESH
F32 = jnp.float32
BF16 = jnp.bfloat16

CH, CIN, SIDE, EDGE, TALL, WIDE = 128, 256, 8, 16, 20, 64
PITCH = 80
BLOCKS = 22
CELLS = BLOCKS * PITCH
BLOCK = 3
OUTER = (1, 2, 19, 20)
DIRS = [(dr, dc) for dr in (-1, 0, 1) for dc in (-1, 0, 1) if (dr, dc) != (0, 0)]

MID = (32, WIDE)
LOW = (0, 32)
HIGH = (WIDE, PITCH)
ALL = (0, PITCH)
TIP = (0, EDGE)
GATE_CORE = [[(4, 11) + MID], [(11, 18) + MID]]
GATE_RIM = [[(2, 4) + ALL, (4, 7) + LOW], [(7, 15) + LOW], [(15, 18) + LOW, (4, 14) + HIGH],
            [(13, 18) + HIGH, (18, 20) + ALL, (20, 21) + TIP]]
CAND_CORE = [[(1, 4) + MID], [(4, 7) + MID]]
CAND_RIM = [[(0, 1) + ALL, (1, 6) + LOW], [(6, 7) + LOW, (1, 7) + HIGH, (7, 8) + ALL, (8, 9) + LOW]]
ZR_CORE = [(336, 272), (608, 272), (880, 288), (1168, 288)]
ZR_RIM = [(160, 176), (1440, 176)]
N_CORE = [[(2, 4) + ALL, (4, 5, 0, 48)], [(4, 5, 32, PITCH), (5, 7) + ALL]]
N_RIM = [[(0, 1) + ALL, (1, 2, 0, 48)], [(1, 2, 48, PITCH), (7, 8) + ALL, (8, 9) + TIP]]


def kernel(n_rows, n_cols, steps, frames, h_init, w_x, w_hzr, w_hn, bias, h_seq, h_last,
           hf, hl, hr, fs, fl, fr, xf, fx, ub, rh, vb, zb, gz, gn, wx, wxn, wh, whn, whr,
           sem_w, sem_f, f_send, f_recv, h_send, h_recv):
    row = lax.axis_index('rows')
    col = lax.axis_index('cols')

    def exists(dr, dc):
        conds = []
        if dr:
            conds.append(row + dr >= 0 if dr < 0 else row + dr < n_rows)
        if dc:
            conds.append(col + dc >= 0 if dc < 0 else col + dc < n_cols)
        return conds[0] if len(conds) == 1 else jnp.logical_and(*conds)

    def peer(dr, dc):
        return {'rows': lax.rem(row + dr + n_rows, n_rows), 'cols': lax.rem(col + dc + n_cols, n_cols)}

    def local_copies():
        return [pltpu.make_async_copy(w_x, wx, sem_w.at[0]), pltpu.make_async_copy(w_hzr, wh, sem_w.at[1]),
                pltpu.make_async_copy(w_hn, whr, sem_w.at[2]),
                pltpu.make_async_copy(h_init.at[0], hf.at[0, 3:19, EDGE:PITCH, :], sem_w.at[3])]

    def frame_copy(t):
        return pltpu.make_async_copy(frames.at[t, 0], fs.at[t, 2:18], sem_f.at[t])

    frame_copy(0).start()
    weights = local_copies()
    weights[3].start()
    weights[0].start()
    for t in range(1, BLOCK):
        frame_copy(t).start()
    weights[1].start()
    weights[2].start()

    barrier = pltpu.get_barrier_semaphore()
    count = jnp.int32(0)
    for d in DIRS:
        here = exists(*d)
        count = count + jnp.where(here, 1, 0)

        @pl.when(here)
        def _(d=d):
            pl.semaphore_signal(barrier, inc=1, device_id=peer(*d), device_id_type=MESH)
    pl.semaphore_wait(barrier, count)

    src_y = {-1: slice(0, 2), 0: slice(0, EDGE), 1: slice(14, EDGE)}
    dst_y = {-1: slice(18, TALL), 0: slice(2, 18), 1: slice(0, 2)}

    def frame_xfer(t, i, local=False):
        dr, dc = DIRS[i]
        cells, land = {0: (slice(0, WIDE), fs), -1: (slice(0, SIDE), fr), 1: (slice(WIDE - SIDE, WIDE), fl)}[dc]
        y = src_y[dr]
        src = fs.at[t, slice(y.start + 2, y.stop + 2), cells] if local else frames.at[t, 0, y, cells]
        return pltpu.make_async_remote_copy(src, land.at[t, dst_y[dr]], f_send.at[t, i], f_recv.at[t, i],
                                            device_id=peer(dr, dc), device_id_type=MESH)

    def state_xfer(t, i, slot):
        dr, dc = DIRS[i]
        k_src = {-1: 3, 0: 3, 1: 17}[dr]
        k_dst = {-1: 19, 0: 3, 1: 1}[dr]
        n = 2 if dr else EDGE
        if slot is None:
            flat = hf.at[t].reshape(BLOCKS * PITCH, CH)
            src = flat.at[pl.ds(PITCH * k_src + SIDE, 2 * PITCH)]
            dst = flat.at[pl.ds(PITCH * k_dst + SIDE, 2 * PITCH)]
        else:
            cells = {0: slice(EDGE, PITCH), -1: slice(EDGE, EDGE + SIDE), 1: slice(PITCH - SIDE, PITCH)}[dc]
            src = hf.at[t, slice(k_src, k_src + n), cells]
            dst = {0: hf.at[t, slice(k_dst, k_dst + n), cells], -1: hr.at[slot, dst_y[dr]], 1: hl.at[slot, dst_y[dr]]}[dc]
        return pltpu.make_async_remote_copy(src, dst, h_send.at[t, i], h_recv.at[t, i], device_id=peer(dr, dc), device_id_type=MESH)

    def start(make, rows_only=False):
        for i, d in enumerate(DIRS):
            if d[1] == 0 or not rows_only:
                @pl.when(exists(*d))
                def _(i=i):
                    make(i).start()

    def finish(make, rows_only=False):
        for i, (dr, dc) in enumerate(DIRS):
            if dc == 0 or not rows_only:
                @pl.when(exists(dr, dc))
                def _(i=i):
                    make(i).wait_send()

                @pl.when(exists(-dr, -dc))
                def _(i=i):
                    make(i).wait_recv()

    frame_copy(0).wait()
    start(lambda i: frame_xfer(0, i, True))
    weights[3].wait()
    start(lambda i: state_xfer(0, i, 0))

    def start_rest(t, carry):
        start(lambda i: frame_xfer(t, i))
        return carry

    for t in range(BLOCK, steps):
        frame_copy(t).start()

    for t in range(steps):
        hf[t, 0, 72:PITCH, :] = jnp.zeros((SIDE, CH), F32)
        hf[t, 1, 0:SIDE, :] = jnp.zeros((SIDE, CH), F32)
        hf[t, 21, SIDE:24, :] = jnp.zeros((EDGE, CH), F32)
    for slot in range(BLOCK):
        for half in range(2):
            xf[slot, half, 72:88, :] = jnp.zeros((EDGE, CH), F32)
            xf[slot, half, 21 * PITCH + SIDE:21 * PITCH + 24, :] = jnp.zeros((EDGE, CH), F32)

    @pl.when(row == 0)
    def _():
        for t in range(steps):
            hf[t, 1, SIDE:PITCH, :] = jnp.zeros((72, CH), F32)
            hf[t, 2, 0:PITCH, :] = jnp.zeros((PITCH, CH), F32)
            hf[t, 3, 0:SIDE, :] = jnp.zeros((SIDE, CH), F32)
            fs[t, 0:2] = jnp.zeros((2, WIDE, CIN), BF16)
            fl[t, 0:2] = jnp.zeros((2, SIDE, CIN), BF16)
            fr[t, 0:2] = jnp.zeros((2, SIDE, CIN), BF16)
        for s in range(2):
            hl[s, 0:2] = jnp.zeros((2, SIDE, CH), F32)
            hr[s, 0:2] = jnp.zeros((2, SIDE, CH), F32)

    @pl.when(row == n_rows - 1)
    def _():
        for t in range(steps):
            hf[t, 19, SIDE:PITCH, :] = jnp.zeros((72, CH), F32)
            hf[t, TALL, 0:PITCH, :] = jnp.zeros((PITCH, CH), F32)
            hf[t, 21, 0:SIDE, :] = jnp.zeros((SIDE, CH), F32)
            fs[t, 18:TALL] = jnp.zeros((2, WIDE, CIN), BF16)
            fl[t, 18:TALL] = jnp.zeros((2, SIDE, CIN), BF16)
            fr[t, 18:TALL] = jnp.zeros((2, SIDE, CIN), BF16)
        for s in range(2):
            hl[s, 18:TALL] = jnp.zeros((2, SIDE, CH), F32)
            hr[s, 18:TALL] = jnp.zeros((2, SIDE, CH), F32)

    @pl.when(col == 0)
    def _():
        for t in range(steps):
            fl[t] = jnp.zeros((TALL, SIDE, CIN), BF16)
        hl[...] = jnp.zeros((2, TALL, SIDE, CH), F32)

    @pl.when(col == n_cols - 1)
    def _():
        for t in range(steps):
            fr[t] = jnp.zeros((TALL, SIDE, CIN), BF16)
        hr[...] = jnp.zeros((2, TALL, SIDE, CH), F32)

    for c in range(3):
        vb[c, 1616:1696, :] = jnp.zeros((PITCH, CH), BF16)
    rh[2 * PITCH - SIDE:2 * PITCH, :] = jnp.zeros((SIDE, CH), F32)
    rh[TALL * PITCH + EDGE:TALL * PITCH + 24, :] = jnp.zeros((SIDE, CH), F32)

    def two_rows(dst, src, depth, lanes):
        zero = jnp.zeros((depth, CH), BF16)
        for c in range(3):
            for a in range(4):
                i = (a * 3 + c) * depth
                dst[i:i + depth, 0:CH] = src[a * 3 + c, :, lanes] if a < 3 else zero
                dst[i:i + depth, CH:2 * CH] = src[a * 3 + c - 3, :, lanes] if a > 0 else zero

    weights[0].wait()
    two_rows(wxn, wx, CIN, slice(2 * CH, 3 * CH))

    def take(ref, boxes):
        parts = [ref[k0:k1, j0:j1, :] for k0, k1, j0, j1 in boxes]
        return jnp.concatenate([x.reshape(-1, x.shape[-1]) for x in parts], axis=0)

    def put(ref, boxes, value):
        at = 0
        for k0, k1, j0, j1 in boxes:
            size = (k1 - k0) * (j1 - j0)
            ref[k0:k1, j0:j1, :] = value[at:at + size].reshape(k1 - k0, j1 - j0, value.shape[-1])
            at += size

    def two_row_patches(ref, depth, boxes):
        taps = []
        for a in range(4):
            lead = 1 + a // 2
            for c in range(3):
                rows = ref.at[c].reshape(BLOCKS // 2, 2, PITCH, depth)
                parts = [rows[y0 + lead:y1 + lead, a % 2, j0:j1, :] for y0, y1, j0, j1 in boxes]
                taps.append(jnp.concatenate([x.reshape(-1, depth) for x in parts], axis=0))
        return jnp.concatenate(taps, axis=1)

    def matmul(lhs, w):
        return jnp.dot(lhs, w, preferred_element_type=F32)

    def shifted(dst, src, lo, hi):
        for c in range(3):
            dst[c, lo:hi, :] = src[lo - 1 + c:hi - 1 + c, :].astype(BF16)

    halves = [(half, slice(half * CH, half * CH + CH)) for half in range(2)]

    def prep_core(t, slot):
        for half, lanes in halves:
            cells = xf.at[slot, half].reshape(BLOCKS, PITCH, CH)
            cells[3:19, EDGE:PITCH, :] = fs[t, 2:18, :, lanes].astype(F32)
            for c in range(3):
                fx[slot, c, 3:19, 32:WIDE, lanes] = cells[3:19, 31 + c:63 + c, :].astype(BF16)

    def prep_rim(t, slot):
        for half, lanes in halves:
            flat = xf.at[slot, half]
            cells = flat.reshape(BLOCKS, PITCH, CH)
            cells[1:3, EDGE:PITCH, :] = fs[t, 0:2, :, lanes].astype(F32)
            cells[19:21, EDGE:PITCH, :] = fs[t, 18:TALL, :, lanes].astype(F32)
            cells[1:21, SIDE:EDGE, :] = fl[t, :, :, lanes].astype(F32)
            cells[2:22, 0:SIDE, :] = fr[t, :, :, lanes].astype(F32)
            for c in range(3):
                out = fx.at[slot, c]
                for k in OUTER:
                    first = PITCH * k - 1 + c
                    out[k, :, lanes] = flat[first:first + PITCH, :].astype(BF16)
                out[21, 0:EDGE, lanes] = flat[PITCH * 21 - 1 + c:PITCH * 21 - 1 + c + EDGE, :].astype(BF16)
                for k in range(3, 19):
                    first = PITCH * k - 1 + c
                    out[k, 0:32, lanes] = flat[first:first + 32, :].astype(BF16)
                    out[k, WIDE:PITCH, lanes] = flat[first + WIDE:first + PITCH, :].astype(BF16)

    def gates(slot, chunks):
        bias_zr = bias[0:2 * CH][None, :]
        wzr = wx[:, :, 0:2 * CH].reshape(9 * CIN, 2 * CH)
        for boxes in chunks:
            taps = [take(fx.at[slot, c], [(k0 + a, k1 + a, j0, j1) for k0, k1, j0, j1 in boxes]) for a in (-1, 0, 1) for c in range(3)]
            put(gz.at[slot], boxes, matmul(jnp.concatenate(taps, axis=1), wzr) + bias_zr)

    def cand_gates(slot, chunks):
        bias_n = bias[2 * CH:3 * CH]
        bias_n = jnp.concatenate([bias_n, bias_n])[None, :]
        for boxes in chunks:
            put(gn.at[slot], boxes, matmul(two_row_patches(fx.at[slot], CIN, boxes), wxn[...]) + bias_n)

    def zr_gates(slot, h_flat, chunks):
        whzr = wh[...].reshape(9 * CH, 2 * CH)
        base = gz.at[slot].reshape(CELLS, 2 * CH)
        for lo, size in chunks:
            here = slice(lo, lo + size)
            taps = [ub[c, lo + a:lo + a + size, :] for a in (-PITCH, 0, PITCH) for c in range(3)]
            gate = 0.5 * jnp.tanh(0.5 * (matmul(jnp.concatenate(taps, axis=1), whzr) + base[here, :])) + 0.5
            zb[here, :] = gate[:, 0:CH]
            rh[here, :] = gate[:, CH:2 * CH] * h_flat[here, :]

    left_edge = col == 0
    right_edge = col == n_cols - 1

    def new_state(t, slot, chunks):
        def rows_of(ref, n):
            return ref.reshape(n // 2, 2, ref.shape[-2], CH)
        old, new = rows_of(hf.at[t].reshape(BLOCKS, PITCH, CH), BLOCKS), rows_of(hf.at[t + 1].reshape(BLOCKS, PITCH, CH), BLOCKS)
        update = zb.reshape(BLOCKS // 2, 2, PITCH, CH)
        seq, final = rows_of(h_seq.at[t, 0], EDGE), rows_of(h_last.at[0], EDGE)
        for boxes in chunks:
            cand = jnp.tanh(matmul(two_row_patches(vb, CH, boxes), whn[...]) + take(gn.at[slot], boxes))
            at = 0
            for y0, y1, j0, j1 in boxes:
                n = (y1 - y0) * (j1 - j0)
                for odd in range(2):
                    if y0 == SIDE and odd:
                        continue
                    ks = slice(y0 + 1 + odd, y1 + 1 + odd)
                    par = 1 - odd
                    z = update[ks, par, j0:j1, :]
                    c = cand[at:at + n, odd * CH:odd * CH + CH].reshape(y1 - y0, j1 - j0, CH)
                    h_new = (1.0 - z) * c + z * old[ks, par, j0:j1, :]
                    lo = max(j0, EDGE)
                    if lo < j1:
                        main = h_new[:, lo - j0:]
                        seq[y0:y1, odd, lo - EDGE:j1 - EDGE, :] = main.astype(BF16)
                        final[y0:y1, odd, lo - EDGE:j1 - EDGE, :] = main
                        new[ks, par, lo:j1, :] = main
                    if j0 == 0 and y0 < SIDE:
                        new[ks, par, SIDE:EDGE, :] = jnp.where(left_edge, 0.0, h_new[:, SIDE:EDGE])
                    if j0 == 0 and (y0 or odd):
                        new[ks, par, 0:SIDE, :] = jnp.where(right_edge, 0.0, h_new[:, 0:SIDE])
                at += n

    def block(b, carry):
        t0 = b * BLOCK

        @pl.when(b == 0)
        def _():
            for t in range(1, BLOCK):
                frame_copy(t).wait()

        @pl.when(b > 0)
        def _():
            for j in range(BLOCK):
                frame_copy(t0 + j).wait()

        for j in range(BLOCK):
            prep_core(t0 + j, j)
            gates(j, GATE_CORE)
        for j in range(BLOCK - 1):
            cand_gates(j, [CAND_CORE[0] + CAND_CORE[1]])
        cand_gates(BLOCK - 1, CAND_CORE)

        @pl.when(b == 0)
        def _():
            lax.fori_loop(1, steps, start_rest, 0)
            weights[1].wait()
            weights[2].wait()
            two_rows(whn, whr, CH, slice(0, CH))

        finish(lambda i: frame_xfer(t0, i))
        prep_rim(t0, 0)
        gates(0, GATE_RIM)
        cand_gates(0, CAND_RIM)
        finish(lambda i: state_xfer(t0, i, b))
        hf[t0, 1:21, SIDE:EDGE, :] = hl[b]
        hf[t0, 2:22, 0:SIDE, :] = hr[b]
        h_flat = hf.at[t0].reshape(CELLS, CH)
        shifted(ub, h_flat, PITCH, 1696)
        zr_gates(0, h_flat, ZR_CORE + ZR_RIM)
        shifted(vb, rh, 160, 1616)
        new_state(t0, 0, N_CORE + N_RIM)
        start(lambda i: state_xfer(t0 + 1, i, None), True)

        for j in range(1, BLOCK):
            t = t0 + j
            finish(lambda i: frame_xfer(t, i))
            h_flat = hf.at[t].reshape(CELLS, CH)
            prep_rim(t, j)
            shifted(ub, h_flat, 256, 1520)
            ends = h_flat[1520:1528, :]
            for c, x in enumerate((h_flat[1519:1527, :], ends, pltpu.roll(ends, SIDE - 1, 0))):
                ub[c, 1520:1528, :] = x.astype(BF16)
            gates(j, GATE_RIM)
            zr_gates(j, h_flat, ZR_CORE)
            shifted(vb, rh, 480, 1440)
            cand_gates(j, CAND_RIM)
            finish(lambda i: state_xfer(t, i, None), True)
            shifted(ub, h_flat, PITCH, 256)
            shifted(ub, h_flat, 1520, 1696)
            zr_gates(j, h_flat, ZR_RIM)
            new_state(t, j, N_CORE[::-1])
            shifted(vb, rh, 160, 480)
            shifted(vb, rh, 1440, 1616)
            new_state(t, j, N_RIM)
            if j < BLOCK - 1:
                start(lambda i: state_xfer(t + 1, i, None), True)
            else:
                @pl.when(b == 0)
                def _():
                    start(lambda i: state_xfer(t + 1, i, 1))
        return carry

    lax.fori_loop(0, steps // BLOCK, block, 0)


def solution(mesh):
    n_rows = mesh.shape['rows']
    n_cols = mesh.shape['cols']
    frame_spec = P(None, 'batch', 'rows', 'cols', None)
    state_spec = P('batch', 'rows', 'cols', None)

    def local_fn(frames, h_init, w_x, w_hzr, w_hn, gate_bias):
        steps = frames.shape[0]
        any_spec = pl.BlockSpec(memory_space=pl.ANY)
        vmem = pltpu.VMEM
        dma = pltpu.SemaphoreType.DMA
        return pl.pallas_call(
            functools.partial(kernel, n_rows, n_cols, steps),
            out_shape=(vmem((steps, 1, EDGE, WIDE, CH), BF16), vmem((1, EDGE, WIDE, CH), F32)),
            in_specs=[any_spec] * 5 + [pl.BlockSpec(memory_space=pltpu.VMEM)],
            out_specs=(pl.BlockSpec(memory_space=vmem), pl.BlockSpec(memory_space=vmem)),
            scratch_shapes=[
                vmem((steps + 1, BLOCKS, PITCH, CH), F32),
                vmem((2, TALL, SIDE, CH), F32),
                vmem((2, TALL, SIDE, CH), F32),
                vmem((steps, TALL, WIDE, CIN), BF16),
                vmem((steps, TALL, SIDE, CIN), BF16),
                vmem((steps, TALL, SIDE, CIN), BF16),
                vmem((BLOCK, 2, BLOCKS * PITCH, CH), F32),
                vmem((BLOCK, 3, BLOCKS, PITCH, CIN), BF16),
                vmem((3, CELLS, CH), BF16),
                vmem((BLOCKS * PITCH, CH), F32),
                vmem((3, CELLS, CH), BF16),
                vmem((CELLS, CH), F32),
                vmem((BLOCK, BLOCKS, PITCH, CIN), F32),
                vmem((BLOCK, 9, PITCH, CIN), F32),
                vmem((9, CIN, 384), BF16),
                vmem((12 * CIN, CIN), BF16),
                vmem((9, CH, CIN), BF16),
                vmem((12 * CH, CIN), BF16),
                vmem((9, CH, CH), BF16),
                dma((4,)), dma((steps,)),
                dma((steps, SIDE)), dma((steps, SIDE)), dma((steps, SIDE)), dma((steps, SIDE)),
            ],
            compiler_params=pltpu.CompilerParams(collective_id=0, has_side_effects=True, vmem_limit_bytes=60 * 1024 * 1024),
        )(frames, h_init, w_x.reshape(9, CIN, 384), w_hzr.reshape(9, CH, CIN), w_hn.reshape(9, CH, CH), gate_bias)

    return jax.shard_map(local_fn, mesh=mesh, in_specs=(frame_spec, state_spec, P(), P(), P(), P()), out_specs=(frame_spec, state_spec), check_vma=False)
```
